32 devices in a mesh: field: 2 (over x), gx: 4 (over z), gy: 4 (over y, core).
Axes of the slice: x: 2, y: 2, z: 4, core: 2. Of those that a mesh axis runs over, the one named last changes fastest.
Arguments:
- concentrations: float32 [2, 16, 16, 32, 128], P('field', None, 'gx', 'gy'), may hold values from 0 to 2
- velocity: float32 [3, 16, 32, 128], P(None, 'gx', 'gy'), may hold values from -0.3 to 0.3
- diffusivity: float32 [16, 32, 128], P('gx', 'gy'), may hold values from 0.02 to 0.12
- wiener: float32 [2, 3, 2, 16, 32, 128], P(None, None, 'field', 'gx', 'gy'), may hold values from -1.8 to 1.8
- mix_rate: float32 [16, 32, 128], P('gx', 'gy'), may hold values from 0.2 to 2
- rate_constants: float32 [64], replicated, may hold values from 0.1 to 1
- reactions: int32 [64, 4], replicated, may hold values from 0 to 15
Outputs:
- advanced: float32 [2, 16, 16, 32, 128], P('field', None, 'gx', 'gy')
The draws below stay inside these ranges and needn't reach their ends.
Inputs may be any that keep to these rules, and one draw needn't show every extreme that they name: `reactions`: each row names two reactant and two product scalars.
All inputs are finite; a program needn't handle non-finite values.
Results may differ from the reference program's by a relative error of at most 0.0001.
Values sent between devices are 32-bit elements; how exact they have to be, the bound alone decides.
No kernel may reach another device: no remote copies, remote signals or barrier semaphores. Data moves between devices by JAX's collectives and lax.ppermute only.
A program may use at most 64 MiB of HBM per device.

```python
import math
import jax
import jax.numpy as jnp
from jax import lax

NS = 16
NR = 64
SUBSTEPS = 12
STEPS = 2
FIELDS = 2
NX = 16
NY = 32
NZ = 128


def plant(values, stream_key, least, top_value):
    extent = values.shape
    place = [jax.random.randint(jax.random.fold_in(stream_key, axis), (), 0, extent[axis]) for axis in range(len(extent))]
    values = values.at[tuple(place)].set(least)
    longest = extent.index(max(extent))
    place[longest] = (place[longest] + 1) % extent[longest]
    return values.at[tuple(place)].set(top_value)


def shard_levels(stream_key, shape, pieces, low, high):
    factor_of = 1.0
    for dim, parts in pieces:
        draws = jax.random.uniform(jax.random.fold_in(jax.random.fold_in(stream_key, 6), dim), (parts,), jnp.float32, low / len(pieces), high / len(pieces))
        factor_of = factor_of * jnp.repeat(jnp.exp(draws), shape[dim] // parts).reshape((-1,) + (1,) * (len(shape) - 1 - dim))
    return factor_of


def scatter_about(key, dims, scale, bound, cuts=(), kind=jnp.bfloat16):
    array = scale * jax.random.normal(key, dims, jnp.float32)
    if cuts:
        array = array * shard_levels(key, dims, cuts, -0.22, 0.18)
    return jnp.clip(array, -bound, bound).astype(kind)


def setup_inputs(seed: int = 0) -> dict:
    seeds = jax.random.split(jax.random.key(seed), 8)
    concentrations = jnp.clip(2.0 * jax.random.uniform(seeds[0], (FIELDS, NS, NX, NY, NZ), jnp.float32) ** shard_levels(seeds[0], (FIELDS, NS, NX, NY, NZ), ((0, 2), (2, 4), (3, 4)), -0.2, 0.2), 0.0, 2.0)
    velocity = jnp.clip(jax.random.uniform(seeds[1], (3, NX, NY, NZ), jnp.float32, -0.3, 0.3) * shard_levels(seeds[1], (3, NX, NY, NZ), ((1, 4), (2, 4)), -0.4, 0.0), -0.3, 0.3)
    diffusivity = jnp.clip(0.02 + 0.09999999776482582 * jax.random.uniform(seeds[2], (NX, NY, NZ), jnp.float32) ** shard_levels(seeds[2], (NX, NY, NZ), ((0, 4), (1, 4)), -0.2, 0.2), 0.02, 0.12)
    wiener = scatter_about(seeds[3], (STEPS, 3, FIELDS, NX, NY, NZ), 0.3, 1.8, ((2, 2), (3, 4), (4, 4)), jnp.float32)
    mix_rate = jnp.clip(jnp.exp(math.log(2.0) - 2.3025851 * jax.random.uniform(seeds[4], (NX, NY, NZ), jnp.float32) ** shard_levels(seeds[4], (NX, NY, NZ), ((0, 4), (1, 4)), -0.2, 0.2)), 0.2, 2.0)
    rate_constants = jnp.clip(jnp.exp(jax.random.uniform(seeds[5], (NR,), jnp.float32, math.log(0.1), math.log(1.0))), 0.1, 1.0)
    reactions = plant(jax.random.randint(seeds[6], (NR, 4), 0, NS), jax.random.fold_in(seeds[6], 1), 0, NS - 1).astype(jnp.int32)
    return {"concentrations": concentrations, "velocity": velocity, "diffusivity": diffusivity, "wiener": wiener, "mix_rate": mix_rate, "rate_constants": rate_constants, "reactions": reactions}


chem_step = 0.04
highest = lax.Precision.HIGHEST

def tables(reactions, count):
    scalar_ids = jnp.arange(count, dtype=jnp.int32)[None, :]
    react = (reactions[:, 0:1] == scalar_ids).astype(jnp.float32) + (reactions[:, 1:2] == scalar_ids).astype(jnp.float32)
    produce = (reactions[:, 2:3] == scalar_ids).astype(jnp.float32) + (reactions[:, 3:4] == scalar_ids).astype(jnp.float32)
    return (react, (produce - react).T)

def neighbours(values):
    middle = (slice(1, -1), slice(1, -1), slice(1, -1))
    leading = (slice(None),) * (values.ndim - 3)
    result = []
    for dim_index in range(3):
        upper_cut = list(middle)
        upper_cut[dim_index] = slice(2, None)
        lower_cut = list(middle)
        lower_cut[dim_index] = slice(0, -2)
        result.append((values[leading + tuple(upper_cut)], values[leading + tuple(lower_cut)]))
    return result

def transport(padded, gamma_pad, gamma, velocity, increments):
    centre = padded[:, 1:-1, 1:-1, 1:-1]
    pairs = neighbours(padded)
    gamma_pairs = neighbours(gamma_pad)
    noise_amp = jnp.sqrt(2.0 * gamma)
    change = jnp.zeros_like(centre)
    for dim_index in range(3):
        upward, downward = pairs[dim_index]
        gamma_up, gamma_down = gamma_pairs[dim_index]
        change = change + 0.5 * (gamma + gamma_up) * (upward - centre) + 0.5 * (gamma + gamma_down) * (downward - centre)
        change = change + (noise_amp * increments[dim_index] - velocity[dim_index]) * (0.5 * (upward - downward))
    return centre + change

def chemistry(values, react, net_t, rate_constants):

    def substep(index, conc):
        logs = jnp.log(jax.nn.softplus(conc))
        flux = rate_constants[:, None] * jnp.exp(jnp.dot(react, logs, precision=highest))
        return conc + chem_step * jnp.dot(net_t, flux, precision=highest)
    return lax.fori_loop(0, SUBSTEPS, substep, values)

def closure(first, second, count, mix_rate):
    mean = first / count
    meansq = second / count
    spread = lax.optimization_barrier(jnp.sum(meansq - mean * mean, axis=0))
    energy = lax.optimization_barrier(jnp.sum(meansq, axis=0))
    omega = mix_rate * (1.0 + spread / (1.0 + energy))
    return (mean, jnp.exp(-0.5 * omega))

def reference(concentrations, velocity, diffusivity, wiener, mix_rate, rate_constants, reactions):
    react, net_t = tables(reactions, NS)
    gamma_pad = jnp.pad(diffusivity, 1)
    conc = concentrations
    for step_index in range(STEPS):

        def advance(pair):
            field_conc, increments = pair
            padded = jnp.pad(field_conc, ((0, 0), (1, 1), (1, 1), (1, 1)))
            moved = transport(padded, gamma_pad, diffusivity, velocity, increments)
            flat = chemistry(moved.reshape(NS, -1), react, net_t, rate_constants)
            return flat.reshape(moved.shape)
        conc = lax.map(advance, (conc, jnp.moveaxis(wiener[step_index], 1, 0)))
        first = lax.optimization_barrier(jnp.sum(conc, axis=0))
        second = lax.optimization_barrier(jnp.sum(conc * conc, axis=0))
        mean, decay = closure(first, second, FIELDS, mix_rate)
        conc = mean + (conc - mean) * decay
    return conc
```

```python
import functools

import jax
import jax.numpy as jnp
from jax import lax
from jax.experimental import pallas as pl
from jax.experimental.pallas import tpu as pltpu
from jax.sharding import PartitionSpec as P

SUBSTEPS = 12
STEPS = 2
CHEM_STEP = 0.04
LOG2E = 1.4426950408889634
LN2 = 0.6931471805599453
TILE = 256
VMEM = pl.BlockSpec(memory_space=pltpu.VMEM)


def roundup(n, m):
    return (n + m - 1) // m * m


def split(x):
    hi = x.astype(jnp.bfloat16)
    lo = (x - hi.astype(jnp.float32)).astype(jnp.bfloat16)
    return hi, lo


def faces_kernel(conc, gamma, reactions, rates, xlo, xhi, ylo, yhi, gather, scatter):
    ns, nx, ny, nz = conc.shape
    nr = reactions.shape[0]
    for s in range(ns):
        xlo[s] = conc[s, 0]
        xhi[s] = conc[s, nx - 1]
        ylo[s] = conc[s, :, 0, :]
        yhi[s] = conc[s, :, ny - 1, :]
    xlo[ns] = gamma[0]
    xhi[ns] = gamma[nx - 1]
    ylo[ns] = gamma[:, 0, :]
    yhi[ns] = gamma[:, ny - 1, :]
    lane = lax.broadcasted_iota(jnp.int32, (nr, 128), 1)
    scalar = lax.rem(lane, ns)
    part = lax.div(lane, ns)
    k = rates[...] * (CHEM_STEP * LN2)
    k_hi = k.astype(jnp.bfloat16).astype(jnp.float32)
    k_lo = k - k_hi
    first = jnp.where(scalar == reactions[:, 0:1], 1.0, 0.0)
    second = jnp.where(scalar == reactions[:, 1:2], 1.0, 0.0)
    weight = jnp.where(part < 2, k_hi, jnp.where(part == 2, k_lo, 0.0))
    gather[:nr, :] = (first * weight).astype(jnp.bfloat16)
    gather[nr:, :] = (second * jnp.where(part < 2, 1.0, 0.0)).astype(jnp.bfloat16)
    third = jnp.where(scalar == reactions[:, 2:3], 1.0, 0.0)
    fourth = jnp.where(scalar == reactions[:, 3:4], 1.0, 0.0)
    net = third + fourth - first - second
    scatter[...] = jnp.concatenate([net, net], axis=0).T[:ns].astype(jnp.bfloat16)


def step_kernel(
    conc, xlo, xhi, ylo, yhi, gamma, glox, ghix, gloy, ghiy, velocity, wiener, gather, scatter,
    out, rows, state
):
    ns, nx, ny, nz = conc.shape
    stride = rows.shape[0] // ns
    chunks = nx * ny
    lane = lax.broadcasted_iota(jnp.int32, (ny, nz), 1)
    sub = lax.broadcasted_iota(jnp.int32, (ny, nz), 0)
    is_top, is_bottom = sub == ny - 1, sub == 0

    def shifted(value, low, high):
        up = jnp.where(is_top, high, pltpu.roll(value, ny - 1, 0))
        down = jnp.where(is_bottom, low, pltpu.roll(value, 1, 0))
        return up, down

    for x in range(nx):
        g = gamma[x]
        amp = jnp.sqrt(2.0 * g)
        gx_up = ghix[ns] if x == nx - 1 else gamma[x + 1]
        gx_down = glox[ns] if x == 0 else gamma[x - 1]
        gy_up, gy_down = shifted(g, gloy[ns, x : x + 1, :], ghiy[ns, x : x + 1, :])
        gz_up = jnp.where(lane == nz - 1, 0.0, pltpu.roll(g, nz - 1, 1))
        gz_down = jnp.where(lane == 0, 0.0, pltpu.roll(g, 1, 1))
        coef = []
        total = jnp.zeros_like(g)
        for d, (gu, gd) in enumerate(((gx_up, gx_down), (gy_up, gy_down), (gz_up, gz_down))):
            drift = 0.5 * (amp * wiener[d, x] - velocity[d, x])
            cu = 0.5 * (g + gu) + drift
            cd = 0.5 * (g + gd) - drift
            total = total + 0.5 * (g + gu) + 0.5 * (g + gd)
            coef.append((cu, cd))
        centre = (1.0 - total) * LOG2E
        (xu, xd), (yu, yd), (zu, zd) = [(a * LOG2E, b * LOG2E) for a, b in coef]
        zu = jnp.where(lane == nz - 1, 0.0, zu)
        zd = jnp.where(lane == 0, 0.0, zd)
        for s in range(ns):
            p = conc[s, x]
            px_up = xhi[s] if x == nx - 1 else conc[s, x + 1]
            px_down = xlo[s] if x == 0 else conc[s, x - 1]
            py_up, py_down = shifted(p, ylo[s, x : x + 1, :], yhi[s, x : x + 1, :])
            pz_up = pltpu.roll(p, nz - 1, 1)
            pz_down = pltpu.roll(p, 1, 1)
            moved = (centre * p + (xu * px_up + xd * px_down)) + (
                (yu * py_up + yd * py_down) + (zu * pz_up + zd * pz_down)
            )
            rows[s * stride + x * ny : s * stride + (x + 1) * ny, :] = moved

    for j in range(chunks):
        state[:, j * nz : (j + 1) * nz] = rows[pl.ds(j, ns, stride=stride), :]

    table = gather[...]
    net = scatter[...]
    nr = table.shape[0] // 2
    depth = 3 * ns
    table = table[:, :depth]

    def substep(i, carry):
        for t in range(chunks * nz // TILE):
            u = state[:, t * TILE : (t + 1) * TILE]
            sp = jnp.maximum(u, jnp.log2(1.0 + jnp.exp2(jnp.minimum(u, 120.0))))
            hi, lo = split(sp)
            both = jnp.dot(
                table,
                jnp.concatenate([hi, lo, hi], axis=0),
                preferred_element_type=jnp.float32,
            )
            rate = both[:nr] * both[nr:]
            hi, lo = split(rate)
            change = jnp.dot(
                net, jnp.concatenate([hi, lo], axis=0), preferred_element_type=jnp.float32
            )
            state[:, t * TILE : (t + 1) * TILE] = u + change
        return carry

    lax.fori_loop(0, SUBSTEPS, substep, 0)

    for j in range(chunks):
        rows[pl.ds(j, ns, stride=stride), :] = state[:, j * nz : (j + 1) * nz] * LN2
    for s in range(ns):
        for x in range(nx):
            out[s, x] = rows[s * stride + x * ny : s * stride + (x + 1) * ny, :]


def mix_kernel(count, mine, other, mix_rate, out, *faces):
    ns, nx, ny, nz = mine.shape
    for x in range(nx):
        spread = jnp.zeros((ny, nz), jnp.float32)
        energy = jnp.zeros((ny, nz), jnp.float32)
        for s in range(ns):
            a, b = mine[s, x], other[s, x]
            mean = (a + b) * (1.0 / count)
            meansq = (a * a + b * b) * (1.0 / count)
            spread = spread + (meansq - mean * mean)
            energy = energy + meansq
        omega = mix_rate[x] * (1.0 + spread / (1.0 + energy))
        decay = jnp.exp(-0.5 * omega)
        for s in range(ns):
            a, b = mine[s, x], other[s, x]
            mean = (a + b) * (1.0 / count)
            new = mean + (a - mean) * decay
            out[s, x] = new
            if faces:
                xlo, xhi, ylo, yhi = faces
                if x == 0:
                    xlo[s] = new
                if x == nx - 1:
                    xhi[s] = new
                ylo[s, x : x + 1] = new[0:1]
                yhi[s, x : x + 1] = new[ny - 1 : ny]


def closure(first, second, count, mix_rate):
    mean = first / count
    meansq = second / count
    spread = jnp.sum(meansq - mean * mean, axis=0)
    energy = jnp.sum(meansq, axis=0)
    omega = mix_rate * (1.0 + spread / (1.0 + energy))
    return (mean, jnp.exp(-0.5 * omega))


def shape_of(*dims, dtype=jnp.float32):
    return jax.ShapeDtypeStruct(dims, dtype)


def exchange(xlo, xhi, ylo, yhi):
    nx, ny = lax.axis_size("gx"), lax.axis_size("gy")
    up = lambda n: [(i, i + 1) for i in range(n - 1)]
    down = lambda n: [(i + 1, i) for i in range(n - 1)]
    from_below = lax.ppermute(xhi, "gx", up(nx))
    from_above = lax.ppermute(xlo, "gx", down(nx))
    from_left = lax.ppermute(yhi, "gy", up(ny))
    from_right = lax.ppermute(ylo, "gy", down(ny))
    return from_below, from_above, from_left, from_right


def on_device(concentrations, velocity, diffusivity, wiener, mix_rate, rate_constants, reactions):
    conc = concentrations[0]
    ns, nx, ny, nz = conc.shape
    nr = reactions.shape[0]
    count = lax.axis_size("field")
    faces = [shape_of(ns, ny, nz), shape_of(ns, ny, nz), shape_of(ns, nx, nz), shape_of(ns, nx, nz)]
    first_faces = [shape_of(ns + 1, *f.shape[1:]) for f in faces]
    *sent, gather, scatter = pl.pallas_call(
        faces_kernel,
        out_shape=first_faces
        + [shape_of(2 * nr, 128, dtype=jnp.bfloat16), shape_of(ns, 2 * nr, dtype=jnp.bfloat16)],
        in_specs=[VMEM] * 4,
        out_specs=[VMEM] * 6,
    )(conc, diffusivity, reactions, rate_constants.reshape(nr, 1))
    stride = roundup(nx * ny, 32) + 1
    halos = exchange(*sent)
    gamma_halos = halos
    for step_index in range(STEPS):
        reacted = pl.pallas_call(
            step_kernel,
            out_shape=shape_of(ns, nx, ny, nz),
            in_specs=[VMEM] * 14,
            out_specs=VMEM,
            scratch_shapes=[
                pltpu.VMEM((ns * stride, nz), jnp.float32),
                pltpu.VMEM((ns, nx * ny * nz), jnp.float32),
            ],
        )(
            conc, *halos, diffusivity, *gamma_halos, velocity, wiener[step_index, :, 0],
            gather, scatter,
        )
        last = step_index == STEPS - 1
        if count == 2:
            other = lax.ppermute(reacted, "field", [(0, 1), (1, 0)])
            mixed = pl.pallas_call(
                functools.partial(mix_kernel, count),
                out_shape=[shape_of(ns, nx, ny, nz)] + ([] if last else faces),
                in_specs=[VMEM] * 3,
                out_specs=[VMEM] * (1 if last else 5),
            )(reacted, other, mix_rate)
            conc, sent = mixed[0], mixed[1:]
        else:
            first = lax.psum(reacted, "field")
            second = lax.psum(reacted * reacted, "field")
            mean, decay = closure(first, second, count, mix_rate)
            conc = mean + (reacted - mean) * decay
            sent = (conc[:, 0], conc[:, -1], conc[:, :, 0], conc[:, :, -1])
        if not last:
            halos = exchange(*sent)
    return conc[None]


def solution(mesh):
    return jax.shard_map(
        on_device,
        mesh=mesh,
        in_specs=(
            P("field", None, "gx", "gy", None),
            P(None, "gx", "gy", None),
            P("gx", "gy", None),
            P(None, None, "field", "gx", "gy", None),
            P("gx", "gy", None),
            P(),
            P(),
        ),
        out_specs=P("field", None, "gx", "gy", None),
        check_vma=False,
    )
```

```python
import functools

import jax
import jax.numpy as jnp
from jax import lax
from jax.experimental import pallas as pl
from jax.experimental.pallas import tpu as pltpu
from jax.sharding import PartitionSpec as P

SUBSTEPS = 12
STEPS = 2
CHEM_STEP = 0.04
LOG2E = 1.4426950408889634
LN2 = 0.6931471805599453
TILE = 256
VMEM = pl.BlockSpec(memory_space=pltpu.VMEM)


def roundup(n, m):
    return (n + m - 1) // m * m


def split(x):
    hi = x.astype(jnp.bfloat16)
    lo = (x - hi.astype(jnp.float32)).astype(jnp.bfloat16)
    return hi, lo


def params(mib):
    return pltpu.CompilerParams(vmem_limit_bytes=mib * 2**20)


def sides(axis):
    here, count = lax.axis_index(axis), lax.axis_size(axis)
    even = lax.rem(here, 2) == 0
    return even, here == 0, here == count - 1


def picked(even, low, high):
    return jnp.where(even, high, low), jnp.where(even, low, high)


def send_faces(conc, s, x1, x2, y1, y2, row):
    nx, ny = conc.shape[-3], conc.shape[-2]
    even, _, _ = sides("gx")
    for ref, x in zip((x1, x2), picked(even, 0, nx - 1)):
        ref[row] = conc[s, x]
    even, _, _ = sides("gy")
    y1[row], y2[row] = picked(even, conc[s, :, 0, :], conc[s, :, ny - 1, :])


def halo(axis, first, second):
    even, lowest, highest = sides(axis)
    above = jnp.where(highest, 0.0, jnp.where(even, first, second))
    below = jnp.where(lowest, 0.0, jnp.where(even, second, first))
    return above, below


def faces_kernel(conc, gamma, x1, x2, y1, y2):
    ns = conc.shape[0]
    for s in range(ns):
        send_faces(conc, s, x1, x2, y1, y2, s)
    send_faces(gamma, 0, x1, x2, y1, y2, ns)


def tables_kernel(ns, reactions, rates, gather, scatter):
    nr = reactions.shape[1]
    depth = gather.shape[1]
    row = lax.broadcasted_iota(jnp.int32, (depth, nr), 0)
    scalar, part = lax.rem(row, ns), lax.div(row, ns)
    k = rates[...] * (CHEM_STEP * LN2)
    k_hi = k.astype(jnp.bfloat16).astype(jnp.float32)
    k_lo = k - k_hi

    def column(c):
        return jnp.where(scalar == reactions[c : c + 1, :], 1.0, 0.0)

    first, second, third, fourth = (column(c) for c in range(4))
    weight = jnp.where(part < 2, k_hi, jnp.where(part == 2, k_lo, 0.0))
    both = jnp.concatenate(
        [first * weight, second * jnp.where(part < 2, 1.0, 0.0)], axis=1
    ).T
    for j in range(nr // 8):
        block = [both[c + 8 * j : c + 8 * j + 8, :] for c in (0, nr)]
        gather[16 * j : 16 * j + 16, :] = jnp.concatenate(block, axis=0).astype(jnp.bfloat16)
    net = (third + fourth - first - second)[:ns].astype(jnp.bfloat16)
    scatter[...] = jnp.concatenate([net, net], axis=1)


def step_kernel(
    step, conc, x1, x2, y1, y2, gamma, gx1, gx2, gy1, gy2, velocity, wiener, gather, scatter,
    out, rows, state
):
    ns, nx, ny, nz = conc.shape
    stride = rows.shape[0] // ns
    chunks = nx * ny
    lane = lax.broadcasted_iota(jnp.int32, (ny, nz), 1)
    sub = lax.broadcasted_iota(jnp.int32, (ny, nz), 0)
    is_top, is_bottom = sub == ny - 1, sub == 0

    def shifted(value, above, below):
        up = jnp.where(is_top, above, pltpu.roll(value, ny - 1, 0))
        down = jnp.where(is_bottom, below, pltpu.roll(value, 1, 0))
        return up, down

    gx_above, gx_below = halo("gx", gx1[ns], gx2[ns])
    gy_above, gy_below = halo("gy", gy1[ns], gy2[ns])
    coefs = []
    for x in range(nx):
        g = gamma[0, x]
        amp = jnp.sqrt(2.0 * g)
        gx_up = gx_above if x == nx - 1 else gamma[0, x + 1]
        gx_down = gx_below if x == 0 else gamma[0, x - 1]
        gy_up, gy_down = shifted(g, gy_above[x : x + 1], gy_below[x : x + 1])
        gz_up = jnp.where(lane == nz - 1, 0.0, pltpu.roll(g, nz - 1, 1))
        gz_down = jnp.where(lane == 0, 0.0, pltpu.roll(g, 1, 1))
        total = jnp.zeros_like(g)
        coef = []
        for d, (gu, gd) in enumerate(((gx_up, gx_down), (gy_up, gy_down), (gz_up, gz_down))):
            drift = 0.5 * (amp * wiener[step, d, 0, x] - velocity[d, x])
            up, down = 0.5 * (g + gu), 0.5 * (g + gd)
            total = total + (up + down)
            coef += [(up + drift) * LOG2E, (down - drift) * LOG2E]
        coef[4] = jnp.where(lane == nz - 1, 0.0, coef[4])
        coef[5] = jnp.where(lane == 0, 0.0, coef[5])
        coefs.append([(1.0 - total) * LOG2E] + coef)
    for s in range(ns):
        x_above, x_below = halo("gx", x1[s], x2[s])
        y_above, y_below = halo("gy", y1[s], y2[s])
        for x in range(nx):
            centre, xu, xd, yu, yd, zu, zd = coefs[x]
            p = conc[s, x]
            px_up = x_above if x == nx - 1 else conc[s, x + 1]
            px_down = x_below if x == 0 else conc[s, x - 1]
            py_up, py_down = shifted(p, y_above[x : x + 1], y_below[x : x + 1])
            pz_up = pltpu.roll(p, nz - 1, 1)
            pz_down = pltpu.roll(p, 1, 1)
            moved = (centre * p + (xu * px_up + xd * px_down)) + (
                (yu * py_up + yd * py_down) + (zu * pz_up + zd * pz_down)
            )
            rows[s * stride + x * ny : s * stride + (x + 1) * ny, :] = moved

    for j in range(chunks):
        state[:, j * nz : (j + 1) * nz] = rows[pl.ds(j, ns, stride=stride), :]
    chemistry(state, gather, scatter)
    for j in range(chunks):
        rows[pl.ds(j, ns, stride=stride), :] = state[:, j * nz : (j + 1) * nz] * LN2
    for s in range(ns):
        for x in range(nx):
            out[s, x] = rows[s * stride + x * ny : s * stride + (x + 1) * ny, :]


def chemistry(state, gather, scatter):
    ns, cells = state.shape
    tiles = cells // TILE
    table, net = gather[...][:, : 3 * ns], scatter[...]
    nr = table.shape[0] // 2
    steps = SUBSTEPS * tiles
    lag = tiles // 2
    both, change = {}, {}

    def cut(t):
        return slice(t % tiles * TILE, (t % tiles + 1) * TILE)

    for t in range(steps + 2 * lag):
        done = t - 2 * lag
        if done >= 0:
            state[:, cut(done)] += change.pop(done)
        if t < steps:
            u = state[:, cut(t)]
            sp = jnp.maximum(u, jnp.log2(1.0 + jnp.exp2(jnp.minimum(u, 120.0))))
            hi, lo = split(sp)
            both[t] = jnp.dot(
                table,
                jnp.concatenate([hi, lo, hi], axis=0),
                preferred_element_type=jnp.float32,
            )
        ready = t - lag
        if 0 <= ready < steps:
            pair = both.pop(ready).reshape(nr // 8, 2, 8, TILE)
            hi, lo = split((pair[:, 0] * pair[:, 1]).reshape(nr, TILE))
            change[ready] = jnp.dot(
                net, jnp.concatenate([hi, lo], axis=0), preferred_element_type=jnp.float32
            )


def mix_kernel(count, mine, other, mix_rate, out, *faces):
    ns, nx, ny, nz = mine.shape
    for x in range(nx):
        spread = jnp.zeros((ny, nz), jnp.float32)
        energy = jnp.zeros((ny, nz), jnp.float32)
        for s in range(ns):
            a, b = mine[s, x], other[s, x]
            mean = (a + b) * (1.0 / count)
            meansq = (a * a + b * b) * (1.0 / count)
            spread = spread + (meansq - mean * mean)
            energy = energy + meansq
        omega = mix_rate[x] * (1.0 + spread / (1.0 + energy))
        decay = jnp.exp(-0.5 * omega)
        for s in range(ns):
            a, b = mine[s, x], other[s, x]
            mean = (a + b) * (1.0 / count)
            new = mean + (a - mean) * decay
            out[s, x] = new
    if faces:
        for s in range(ns):
            send_faces(out, s, *faces, s)


def closure(first, second, count, mix_rate):
    mean = first / count
    meansq = second / count
    spread = jnp.sum(meansq - mean * mean, axis=0)
    energy = jnp.sum(meansq, axis=0)
    omega = mix_rate * (1.0 + spread / (1.0 + energy))
    return (mean, jnp.exp(-0.5 * omega))


def shape_of(*dims, dtype=jnp.float32):
    return jax.ShapeDtypeStruct(dims, dtype)


def swaps(count):
    pairs = [[(i, i + 1) for i in range(start, count - 1, 2)] for start in (0, 1)]
    return [(p, sorted(set(range(count)) - {i for q in p for i in q})) for p in pairs]


def swap(value, axis, pairs, rest, other=None):
    both = pairs + [(j, i) for i, j in pairs]
    if other is not None and rest and lax.axis_size(other) % 2 == 0:
        n = lax.axis_size(other)
        joint = [(i * n + k, j * n + k) for i, j in both for k in range(n)]
        joint += [(i * n + k, i * n + k + 1 - 2 * (k % 2)) for i in rest for k in range(n)]
        return lax.ppermute(value, (axis, other), joint)
    if len(rest) == 2:
        both = both + [tuple(rest), tuple(rest[::-1])]
    else:
        both = both + [(i, i) for i in rest]
    return lax.ppermute(value, axis, both)


def exchange(x1, x2, y1, y2):
    (a, rest_a), (b, rest_b) = swaps(lax.axis_size("gx"))
    (c, rest_c), (d, rest_d) = swaps(lax.axis_size("gy"))
    return (
        swap(x1, "gx", a, rest_a, "gy"),
        swap(x2, "gx", b, rest_b, "gy"),
        swap(y1, "gy", c, rest_c),
        swap(y2, "gy", d, rest_d),
    )


def on_device(concentrations, velocity, diffusivity, wiener, mix_rate, rate_constants, reactions):
    conc = concentrations[0]
    ns, nx, ny, nz = conc.shape
    nr = reactions.shape[0]
    count = lax.axis_size("field")
    gamma = diffusivity[None]
    face_dims = [(ny, nz), (ny, nz), (nx, nz), (nx, nz)]
    sent = pl.pallas_call(
        faces_kernel,
        out_shape=[shape_of(ns + 1, *d) for d in face_dims],
        in_specs=[VMEM] * 2,
        out_specs=[VMEM] * 4,
        compiler_params=params(4),
        name="faces",
    )(conc, gamma)
    gather, scatter = pl.pallas_call(
        functools.partial(tables_kernel, ns),
        out_shape=[
            shape_of(2 * nr, 128, dtype=jnp.bfloat16), shape_of(ns, 2 * nr, dtype=jnp.bfloat16)
        ],
        in_specs=[VMEM] * 2,
        out_specs=[VMEM] * 2,
        compiler_params=params(2),
        name="tables",
    )(reactions.T, rate_constants.reshape(1, nr))
    stride = roundup(nx * ny, 32) + 1
    halos = exchange(*sent)
    gamma_halos = halos
    for step_index in range(STEPS):
        reacted = pl.pallas_call(
            functools.partial(step_kernel, step_index),
            out_shape=shape_of(ns, nx, ny, nz),
            in_specs=[VMEM] * 14,
            out_specs=VMEM,
            scratch_shapes=[
                pltpu.VMEM((ns * stride, nz), jnp.float32),
                pltpu.VMEM((ns, nx * ny * nz), jnp.float32),
            ],
            compiler_params=params(8),
            name="step",
        )(
            conc, *halos, gamma, *gamma_halos, velocity, wiener, gather, scatter,
        )
        last = step_index == STEPS - 1
        if count == 2:
            other = lax.ppermute(reacted, "field", [(0, 1), (1, 0)])
            mixed = pl.pallas_call(
                functools.partial(mix_kernel, count),
                out_shape=[shape_of(ns, nx, ny, nz)]
                + ([] if last else [shape_of(ns, *d) for d in face_dims]),
                in_specs=[VMEM] * 3,
                out_specs=[VMEM] * (1 if last else 5),
                compiler_params=params(4),
                name="mix",
            )(reacted, other, mix_rate)
            conc, sent = mixed[0], mixed[1:]
        else:
            first = lax.psum(reacted, "field")
            second = lax.psum(reacted * reacted, "field")
            mean, decay = closure(first, second, count, mix_rate)
            conc = mean + (reacted - mean) * decay
            if not last:
                x_even, y_even = sides("gx")[0], sides("gy")[0]
                sent = picked(x_even, conc[:, 0], conc[:, -1]) + picked(
                    y_even, conc[:, :, 0], conc[:, :, -1]
                )
        if not last:
            halos = exchange(*sent)
    return conc[None]


def solution(mesh):
    return jax.shard_map(
        on_device,
        mesh=mesh,
        in_specs=(
            P("field", None, "gx", "gy", None),
            P(None, "gx", "gy", None),
            P("gx", "gy", None),
            P(None, None, "field", "gx", "gy", None),
            P("gx", "gy", None),
            P(),
            P(),
        ),
        out_specs=P("field", None, "gx", "gy", None),
        check_vma=False,
    )
```

```python
import functools

import jax
import jax.numpy as jnp
from jax import lax
from jax.experimental import pallas as pl
from jax.experimental.pallas import tpu as pltpu
from jax.sharding import PartitionSpec as P

SUBSTEPS = 12
STEPS = 2
CHEM_STEP = 0.04
LOG2E = 1.4426950408889634
LN2 = 0.6931471805599453
TILE = 256
VMEM = pl.BlockSpec(memory_space=pltpu.VMEM)
HBM = pl.BlockSpec(memory_space=pltpu.HBM)


def roundup(n, m):
    return (n + m - 1) // m * m


def split(x):
    hi = x.astype(jnp.bfloat16)
    lo = (x - hi.astype(jnp.float32)).astype(jnp.bfloat16)
    return hi, lo


def shape_of(*dims, dtype=jnp.float32):
    return jax.ShapeDtypeStruct(dims, dtype)


def call(kernel, name, mib, out_shape, *args, in_specs=None, scratch_shapes=()):
    return pl.pallas_call(
        kernel,
        out_shape=out_shape,
        in_specs=in_specs or [VMEM] * len(args),
        out_specs=[VMEM] * len(out_shape),
        scratch_shapes=scratch_shapes,
        compiler_params=pltpu.CompilerParams(vmem_limit_bytes=mib * 2**20),
        name=name,
    )(*args)


def swaps(count):
    pairs = [[(i, i + 1) for i in range(start, count - 1, 2)] for start in (0, 1)]
    return [(p, sorted(set(range(count)) - {i for q in p for i in q})) for p in pairs]


def swap(value, axis, pairs, rest, other=None):
    both = pairs + [(j, i) for i, j in pairs]
    if other is not None and rest and lax.axis_size(other) % 2 == 0:
        n = lax.axis_size(other)
        joint = [(i * n + k, j * n + k) for i, j in both for k in range(n)]
        joint += [(i * n + k, i * n + k + 1 - 2 * (k % 2)) for i in rest for k in range(n)]
        return lax.ppermute(value, (axis, other), joint)
    if len(rest) == 2:
        both = both + [tuple(rest), tuple(rest[::-1])]
    else:
        both = both + [(i, i) for i in rest]
    return lax.ppermute(value, axis, both)


def exchange(x1, x2, y1, y2):
    (a, rest_a), (b, rest_b) = swaps(lax.axis_size("gx"))
    (c, rest_c), (d, rest_d) = swaps(lax.axis_size("gy"))
    return (
        swap(x1, "gx", a, rest_a, "gy"),
        swap(x2, "gx", b, rest_b, "gy"),
        swap(y1, "gy", c, rest_c),
        swap(y2, "gy", d, rest_d),
    )


def sides(axis):
    here, count = lax.axis_index(axis), lax.axis_size(axis)
    even = lax.rem(here, 2) == 0
    return even, here == 0, here == count - 1


def picked(even, low, high):
    return jnp.where(even, high, low), jnp.where(even, low, high)


def send_faces(conc, s, x1, x2, y1, y2, row):
    nx, ny = conc.shape[-3], conc.shape[-2]
    even, _, _ = sides("gx")
    for ref, x in zip((x1, x2), picked(even, 0, nx - 1)):
        ref[row] = conc[s, x]
    even, _, _ = sides("gy")
    y1[row], y2[row] = picked(even, conc[s, :, 0, :], conc[s, :, ny - 1, :])


def halo(axis, first, second):
    even, lowest, highest = sides(axis)
    above = jnp.where(highest, 0.0, jnp.where(even, first, second))
    below = jnp.where(lowest, 0.0, jnp.where(even, second, first))
    return above, below


def lanes(like):
    return lax.broadcasted_iota(jnp.int32, like, len(like) - 1)


def kept(dims):
    half = dims[-1] // 2
    return (lanes(dims) >= half) == (lax.axis_index("field") == 1)


def turned(value):
    return pltpu.roll(value, value.shape[-1] // 2, value.ndim - 1)


def doubled(value):
    return jnp.where(kept(value.shape), value, turned(value))


def packed(low, high, mask):
    return jnp.where(mask, low, turned(high))


def shifted(value, above, below):
    ny = value.shape[0]
    sub = lax.broadcasted_iota(jnp.int32, value.shape, 0)
    up = jnp.where(sub == ny - 1, above, pltpu.roll(value, ny - 1, 0))
    down = jnp.where(sub == 0, below, pltpu.roll(value, 1, 0))
    return up, down


def means(gamma, x1, x2, y1, y2):
    nx, ny, nz = gamma.shape
    last = x1.shape[0] - 1
    lane = lanes((ny, nz))
    x_above, x_below = halo("gx", x1[last], x2[last])
    y_above, y_below = halo("gy", y1[last], y2[last])
    result = []
    for x in range(nx):
        g = gamma[x]
        pairs = [
            (
                x_above if x == nx - 1 else gamma[x + 1],
                x_below if x == 0 else gamma[x - 1],
            ),
            shifted(g, y_above[x : x + 1], y_below[x : x + 1]),
            (
                jnp.where(lane == nz - 1, 0.0, pltpu.roll(g, nz - 1, 1)),
                jnp.where(lane == 0, 0.0, pltpu.roll(g, 1, 1)),
            ),
        ]
        result.append([(0.5 * (g + up), 0.5 * (g + down)) for up, down in pairs])
    return result


def stencil(pairs, drifts, top, bottom):
    total = sum(up + down for up, down in pairs)
    coef = [(1.0 - total) * LOG2E]
    for (up, down), drift in zip(pairs, drifts):
        coef += [(up + drift) * LOG2E, (down - drift) * LOG2E]
    coef[5] = jnp.where(top, 0.0, coef[5])
    coef[6] = jnp.where(bottom, 0.0, coef[6])
    return coef


def move(conc, s, coefs, x1, x2, y1, y2, along_z):
    nx = conc.shape[1]
    x_above, x_below = halo("gx", x1[s], x2[s])
    y_above, y_below = halo("gy", y1[s], y2[s])
    for x in range(nx):
        centre, xu, xd, yu, yd, zu, zd = coefs[x]
        p = conc[s, x]
        px_up = x_above if x == nx - 1 else conc[s, x + 1]
        px_down = x_below if x == 0 else conc[s, x - 1]
        py_up, py_down = shifted(p, y_above[x : x + 1], y_below[x : x + 1])
        pz_up, pz_down = along_z(p, s * nx + x)
        yield (centre * p + (xu * px_up + xd * px_down)) + (
            (yu * py_up + yd * py_down) + (zu * pz_up + zd * pz_down)
        )


def whole_z(p, item):
    nz = p.shape[1]
    return pltpu.roll(p, nz - 1, 1), pltpu.roll(p, 1, 1)


def chemistry(state, gather, scatter):
    ns, cells = state.shape
    tiles = cells // TILE
    table, net = gather[...][:, : 3 * ns], scatter[...]
    nr = table.shape[0] // 2
    steps = SUBSTEPS * tiles
    lag = tiles // 2
    both, change = {}, {}

    def cut(t):
        return slice(t % tiles * TILE, (t % tiles + 1) * TILE)

    for t in range(steps + 2 * lag):
        done = t - 2 * lag
        if done >= 0:
            state[:, cut(done)] += change.pop(done)
        if t < steps:
            u = state[:, cut(t)]
            sp = jnp.maximum(u, jnp.log2(1.0 + jnp.exp2(jnp.minimum(u, 120.0))))
            hi, lo = split(sp)
            both[t] = jnp.dot(
                table,
                jnp.concatenate([hi, lo, hi], axis=0),
                preferred_element_type=jnp.float32,
            )
        ready = t - lag
        if 0 <= ready < steps:
            pair = both.pop(ready).reshape(nr // 8, 2, 8, TILE)
            hi, lo = split((pair[:, 0] * pair[:, 1]).reshape(nr, TILE))
            change[ready] = jnp.dot(
                net, jnp.concatenate([hi, lo], axis=0), preferred_element_type=jnp.float32
            )


def react(rows, state, gather, scatter):
    ns = state.shape[0]
    nz = rows.shape[1]
    stride = rows.shape[0] // ns
    chunks = state.shape[1] // nz
    for j in range(chunks):
        state[:, j * nz : (j + 1) * nz] = rows[pl.ds(j, ns, stride=stride), :]
    chemistry(state, gather, scatter)
    for j in range(chunks):
        rows[pl.ds(j, ns, stride=stride), :] = state[:, j * nz : (j + 1) * nz] * LN2


def scratch(ns, nx, ny, nz):
    stride = roundup(nx * ny, 32) + 1
    return [
        pltpu.VMEM((ns * stride, nz), jnp.float32),
        pltpu.VMEM((ns, nx * ny * nz), jnp.float32),
    ]


def mixing(pairs, count, mix_rate):
    ns, get = pairs
    spread, energy = jnp.zeros_like(mix_rate), jnp.zeros_like(mix_rate)
    for s in range(ns):
        a, b = get(s)
        mean = (a + b) * (1.0 / count)
        meansq = (a * a + b * b) * (1.0 / count)
        spread = spread + (meansq - mean * mean)
        energy = energy + meansq
    decay = jnp.exp(-0.5 * (mix_rate * (1.0 + spread / (1.0 + energy))))
    for s in range(ns):
        a, b = get(s)
        mean = (a + b) * (1.0 / count)
        yield mean + (a - mean) * decay, mean + (b - mean) * decay


def faces_kernel(conc_in, gamma_in, x1, x2, y1, y2, conc, gamma, sems):
    ns = conc.shape[0]
    copies = [
        pltpu.make_async_copy(conc_in, conc, sems.at[0]),
        pltpu.make_async_copy(gamma_in, gamma, sems.at[1]),
    ]
    for copy in copies:
        copy.start()
    for copy in copies:
        copy.wait()
    for s in range(ns):
        send_faces(conc, s, x1, x2, y1, y2, s)
    send_faces(gamma, 0, x1, x2, y1, y2, ns)


def tables_kernel(ns, reactions, rates, gather, scatter):
    nr = reactions.shape[1]
    depth = gather.shape[1]
    row = lax.broadcasted_iota(jnp.int32, (depth, nr), 0)
    scalar, part = lax.rem(row, ns), lax.div(row, ns)
    k = rates[...] * (CHEM_STEP * LN2)
    k_hi = k.astype(jnp.bfloat16).astype(jnp.float32)
    k_lo = k - k_hi

    def column(c):
        return jnp.where(scalar == reactions[c : c + 1, :], 1.0, 0.0)

    first, second, third, fourth = (column(c) for c in range(4))
    weight = jnp.where(part < 2, k_hi, jnp.where(part == 2, k_lo, 0.0))
    both = jnp.concatenate(
        [first * weight, second * jnp.where(part < 2, 1.0, 0.0)], axis=1
    ).T
    for j in range(nr // 8):
        block = [both[c + 8 * j : c + 8 * j + 8, :] for c in (0, nr)]
        gather[16 * j : 16 * j + 16, :] = jnp.concatenate(block, axis=0).astype(jnp.bfloat16)
    net = (third + fourth - first - second)[:ns].astype(jnp.bfloat16)
    scatter[...] = jnp.concatenate([net, net], axis=1)


def prepare_kernel(
    ns, reactions, rates, gamma, velocity, wiener, mix_rate,
    gather, scatter, drift, amp, speed, noise, noise_out, mix_packed, mix_doubled
):
    tables_kernel(ns, reactions, rates, gather, scatter)
    nx = gamma.shape[1]
    own = kept(gamma.shape[2:])
    for x in range(nx):
        root = jnp.sqrt(2.0 * gamma[0, x])
        amp[x] = doubled(root)
        mix_doubled[x] = doubled(mix_rate[x])
        for d in range(3):
            drift[d, x] = 0.5 * (root * wiener[0, d, 0, x] - velocity[d, x])
            speed[d, x] = doubled(velocity[d, x])
            noise[d, x] = wiener[1, d, 0, x]
    for x in range(nx // 2):
        mix_packed[x] = packed(mix_rate[x], mix_rate[x + nx // 2], own)
        for d in range(3):
            noise_out[d * (nx // 2) + x] = packed(
                wiener[1, d, 0, x], wiener[1, d, 0, x + nx // 2], jnp.logical_not(own)
            )


def leave_kernel(conc, x1, x2, y1, y2, gamma, drift, mine, theirs):
    ns, nx, ny, nz = conc.shape
    own = kept((ny, nz))
    lane = lanes((ny, nz))
    pairs = means(gamma.at[0], x1, x2, y1, y2)
    coefs = [
        stencil(pairs[x], [drift[d, x] for d in range(3)], lane == nz - 1, lane == 0)
        for x in range(nx)
    ]
    for s in range(ns):
        moved = list(move(conc, s, coefs, x1, x2, y1, y2, whole_z))
        for x in range(nx // 2):
            mine[s, x] = packed(moved[x], moved[x + nx // 2], own)
            theirs[s, x] = packed(moved[x], moved[x + nx // 2], jnp.logical_not(own))


def coefs_kernel(gamma, x1, x2, y1, y2, ups, downs):
    pairs = means(gamma.at[0], x1, x2, y1, y2)
    for x, plane in enumerate(pairs):
        for d, (up, down) in enumerate(plane):
            ups[d, x] = doubled(up)
            downs[d, x] = doubled(down)


def first_kernel(
    count, mine, theirs, gather, scatter, mix_rate, noise_out,
    conc, x1, x2, y1, y2, side, rows, state
):
    ns, nx, ny, nz = conc.shape
    half = nx // 2
    stride = rows.shape[0] // ns
    own = kept((ny, nz))
    is_first = lax.axis_index("field") == 0

    def place(s, field, x):
        start = s * stride + (field * half + x) * ny
        return slice(start, start + ny)

    for s in range(ns):
        for x in range(half):
            rows[place(s, 0, x), :] = mine[s, x]
            rows[place(s, 1, x), :] = theirs[s, x]
    react(rows, state, gather, scatter)
    for x in range(half):
        mixed = mixing(
            (ns, lambda s: (rows[place(s, 0, x), :], rows[place(s, 1, x), :])),
            count,
            mix_rate[x],
        )
        for s, (a, b) in enumerate(mixed):
            conc[s, x] = packed(a, b, own)
            conc[s, x + half] = jnp.where(own, turned(a), b)
    per = nz // 2
    lane = lax.rem(lanes((ny, nz)), per)
    parts = side.shape[0] - noise_out.shape[0]
    for part in range(parts):
        column = jnp.zeros((ny, nz), jnp.float32)
        for item in range(part * per, min(ns * nx, (part + 1) * per)):
            j = item % per
            shift = jnp.where(is_first, (j + per + 1) % nz, j)
            value = pltpu.roll(conc[item // nx, item % nx], shift, 1)
            column = jnp.where(lane == j, value, column)
        side[part] = column
    side[parts:] = noise_out[...]
    for s in range(ns):
        send_faces(conc, s, x1, x2, y1, y2, s)


def second_kernel(
    count, conc, x1, x2, y1, y2, side, ups, downs, amp, speed, noise, gather, scatter, mix_rate,
    mine, theirs, rows, state
):
    ns, nx, ny, nz = conc.shape
    half, per = nx // 2, nz // 2
    stride = rows.shape[0] // ns
    own = kept((ny, nz))
    is_first = lax.axis_index("field") == 0
    lane = lax.rem(lanes((ny, nz)), per)
    at_top, at_bottom = lane == per - 1, lane == 0
    top = jnp.logical_and(at_top, jnp.logical_not(is_first))
    bottom = jnp.logical_and(at_bottom, is_first)
    parts = side.shape[0] - 3 * half

    def half_z(p, item):
        j = item % per
        shift = jnp.where(is_first, per - 1 - j, (nz - j) % nz)
        edge = pltpu.roll(side[item // per], shift, 1)
        up, down = whole_z(p, item)
        return jnp.where(at_top, edge, up), jnp.where(at_bottom, edge, down)

    coefs = []
    for x in range(nx):
        drifts = []
        for d in range(3):
            got = side[parts + d * half + x % half]
            other = turned(got) if x < half else got
            drifts.append(0.5 * (amp[x] * jnp.where(own, noise[d, x], other) - speed[d, x]))
        pairs = [(ups[d, x], downs[d, x]) for d in range(3)]
        coefs.append(stencil(pairs, drifts, top, bottom))
    for s in range(ns):
        for x, moved in enumerate(move(conc, s, coefs, x1, x2, y1, y2, half_z)):
            rows[s * stride + x * ny : s * stride + (x + 1) * ny, :] = moved
    react(rows, state, gather, scatter)

    def field_pair(x):
        def get(s):
            a = rows[s * stride + x * ny : s * stride + (x + 1) * ny, :]
            return a, turned(a)

        return get

    for x in range(half):
        low = mixing((ns, field_pair(x)), count, mix_rate[x])
        high = mixing((ns, field_pair(x + half)), count, mix_rate[x + half])
        for s, ((a, _), (b, _)) in enumerate(zip(low, high)):
            mine[s, x] = a
            mine[s, x + half] = b
            theirs[s, x] = packed(a, b, jnp.logical_not(own))


def join_kernel(mine, theirs, out):
    ns, nx, ny, nz = mine.shape
    half = nx // 2
    own = kept((ny, nz))
    for s in range(ns):
        for x in range(half):
            out[s, x] = packed(mine[s, x], theirs[s, x], own)
            out[s, x + half] = jnp.where(own, mine[s, x + half], theirs[s, x])


def step_kernel(
    step, conc, x1, x2, y1, y2, gamma, gx1, gx2, gy1, gy2, velocity, wiener, gather, scatter,
    out, rows, state
):
    ns, nx, ny, nz = conc.shape
    stride = rows.shape[0] // ns
    lane = lanes((ny, nz))
    pairs = means(gamma.at[0], gx1, gx2, gy1, gy2)
    coefs = []
    for x in range(nx):
        amp = jnp.sqrt(2.0 * gamma[0, x])
        drifts = [0.5 * (amp * wiener[step, d, 0, x] - velocity[d, x]) for d in range(3)]
        coefs.append(stencil(pairs[x], drifts, lane == nz - 1, lane == 0))
    for s in range(ns):
        for x, moved in enumerate(move(conc, s, coefs, x1, x2, y1, y2, whole_z)):
            rows[s * stride + x * ny : s * stride + (x + 1) * ny, :] = moved
    react(rows, state, gather, scatter)
    for s in range(ns):
        for x in range(nx):
            out[s, x] = rows[s * stride + x * ny : s * stride + (x + 1) * ny, :]


def closure(first, second, count, mix_rate):
    mean = first / count
    meansq = second / count
    spread = jnp.sum(meansq - mean * mean, axis=0)
    energy = jnp.sum(meansq, axis=0)
    omega = mix_rate * (1.0 + spread / (1.0 + energy))
    return (mean, jnp.exp(-0.5 * omega))


def on_device(concentrations, velocity, diffusivity, wiener, mix_rate, rate_constants, reactions):
    ns, nx, ny, nz = concentrations.shape[1:]
    nr = reactions.shape[0]
    count = lax.axis_size("field")
    rates = rate_constants.reshape(1, nr)
    table_shapes = [
        shape_of(2 * nr, 128, dtype=jnp.bfloat16), shape_of(ns, 2 * nr, dtype=jnp.bfloat16)
    ]
    face_dims = [(ny, nz), (ny, nz), (nx, nz), (nx, nz)]
    faces = [shape_of(ns, *d) for d in face_dims]
    block = shape_of(ns, nx, ny, nz)
    *sent, conc, gamma = call(
        faces_kernel, "faces", 4,
        [shape_of(ns + 1, *d) for d in face_dims] + [block, shape_of(1, nx, ny, nz)],
        concentrations[0], diffusivity[None],
        in_specs=[HBM] * 2, scratch_shapes=[pltpu.SemaphoreType.DMA((2,))],
    )
    halos = exchange(*sent)
    if count == 2 and STEPS == 2 and nx % 2 == 0 and nz == 128:
        half = shape_of(ns, nx // 2, ny, nz)
        partner = [(0, 1), (1, 0)]
        vectors, planes = shape_of(3, nx, ny, nz), shape_of(nx, ny, nz)
        noise_dims = 3 * (nx // 2)
        gather, scatter, drift, amp, speed, noise, noise_out, mix_packed, mix_doubled = call(
            functools.partial(prepare_kernel, ns), "prepare", 4,
            table_shapes
            + [vectors, planes, vectors, vectors, shape_of(noise_dims, ny, nz)]
            + [shape_of(nx // 2, ny, nz), planes],
            reactions.T, rates, gamma, velocity, wiener, mix_rate,
        )
        mine, theirs = call(
            leave_kernel, "leave", 4, [half, half], conc, *halos, gamma, drift
        )
        theirs = lax.ppermute(theirs, "field", partner)
        ups, downs = call(coefs_kernel, "coefs", 4, [vectors, vectors], gamma, *halos)
        parts = -(-ns * nx // (nz // 2))
        conc, *sent, side = call(
            functools.partial(first_kernel, count), "first", 8,
            [block] + faces + [shape_of(parts + noise_dims, ny, nz)],
            mine, theirs, gather, scatter, mix_packed, noise_out,
            scratch_shapes=scratch(ns, nx, ny, nz),
        )
        halos = exchange(*sent)
        side = lax.ppermute(side, "field", partner)
        mine, theirs = call(
            functools.partial(second_kernel, count), "second", 8, [block, half],
            conc, *halos, side, ups, downs, amp, speed, noise, gather, scatter, mix_doubled,
            scratch_shapes=scratch(ns, nx, ny, nz),
        )
        theirs = lax.ppermute(theirs, "field", partner)
        (out,) = call(join_kernel, "join", 4, [block], mine, theirs)
        return out[None]
    gather, scatter = call(
        functools.partial(tables_kernel, ns), "tables", 2, table_shapes, reactions.T, rates
    )
    gamma_halos = halos
    for step_index in range(STEPS):
        (reacted,) = call(
            functools.partial(step_kernel, step_index), "step", 8, [block],
            conc, *halos, gamma, *gamma_halos, velocity, wiener, gather, scatter,
            scratch_shapes=scratch(ns, nx, ny, nz),
        )
        first = lax.psum(reacted, "field")
        second = lax.psum(reacted * reacted, "field")
        mean, decay = closure(first, second, count, mix_rate)
        conc = mean + (reacted - mean) * decay
        if step_index < STEPS - 1:
            sent = picked(sides("gx")[0], conc[:, 0], conc[:, -1])
            sent += picked(sides("gy")[0], conc[:, :, 0], conc[:, :, -1])
            halos = exchange(*sent)
    return conc[None]


def solution(mesh):
    return jax.shard_map(
        on_device,
        mesh=mesh,
        in_specs=(
            P("field", None, "gx", "gy", None),
            P(None, "gx", "gy", None),
            P("gx", "gy", None),
            P(None, None, "field", "gx", "gy", None),
            P("gx", "gy", None),
            P(),
            P(),
        ),
        out_specs=P("field", None, "gx", "gy", None),
        check_vma=False,
    )
```

```python
import functools

import jax
import jax.numpy as jnp
from jax import lax
from jax.experimental import pallas as pl
from jax.experimental.pallas import tpu as pltpu
from jax.sharding import PartitionSpec as P


SUBSTEPS = 12
STEPS = 2
CHEM_STEP = 0.04
LOG2E = 1.4426950408889634
LN2 = 0.6931471805599453
TILE = 256
VMEM = pl.BlockSpec(memory_space=pltpu.VMEM)
HBM = pl.BlockSpec(memory_space=pltpu.HBM)


def roundup(n, m):
    return (n + m - 1) // m * m


def split(x):
    hi = x.astype(jnp.bfloat16)
    lo = (x - hi.astype(jnp.float32)).astype(jnp.bfloat16)
    return hi, lo


def shape_of(*dims, dtype=jnp.float32):
    return jax.ShapeDtypeStruct(dims, dtype)


def call(kernel, mib, out_shape, *args, in_specs=None, scratch_shapes=()):
    return pl.pallas_call(
        kernel,
        out_shape=out_shape,
        in_specs=in_specs or [VMEM] * len(args),
        out_specs=[VMEM] * len(out_shape),
        scratch_shapes=scratch_shapes,
        compiler_params=pltpu.CompilerParams(vmem_limit_bytes=mib * 2**20),
    )(*args)


def swaps(count):
    pairs = [[(i, i + 1) for i in range(start, count - 1, 2)] for start in (0, 1)]
    return [(p, sorted(set(range(count)) - {i for q in p for i in q})) for p in pairs]


def swap(value, axis, pairs, rest, other=None):
    both = pairs + [(j, i) for i, j in pairs]
    if other is not None and rest and lax.axis_size(other) % 2 == 0:
        n = lax.axis_size(other)
        joint = [(i * n + k, j * n + k) for i, j in both for k in range(n)]
        joint += [(i * n + k, i * n + k + 1 - 2 * (k % 2)) for i in rest for k in range(n)]
        return lax.ppermute(value, (axis, other), joint)
    if len(rest) == 2:
        both = both + [tuple(rest), tuple(rest[::-1])]
    else:
        both = both + [(i, i) for i in rest]
    return lax.ppermute(value, axis, both)


def exchange(x1, x2, y1, y2):
    (a, rest_a), (b, rest_b) = swaps(lax.axis_size("gx"))
    (c, rest_c), (d, rest_d) = swaps(lax.axis_size("gy"))
    x1 = swap(x1, "gx", a, rest_a, "gy")
    x2 = swap(x2, "gx", b, rest_b, "gy")
    y1 = swap(y1, "gy", c, rest_c)
    y2 = swap(y2, "gy", d, rest_d)
    return x1, x2, y1, y2


def sides(axis):
    here, count = lax.axis_index(axis), lax.axis_size(axis)
    even = lax.rem(here, 2) == 0
    return even, here == 0, here == count - 1


def picked(even, low, high):
    return jnp.where(even, high, low), jnp.where(even, low, high)


def send_faces(conc, s, x1, x2, y1, y2, row):
    nx, ny = conc.shape[-3], conc.shape[-2]
    even, _, _ = sides("gx")
    for ref, x in zip((x1, x2), picked(even, 0, nx - 1)):
        ref[row] = conc[s, x]
    even, _, _ = sides("gy")
    y1[row], y2[row] = picked(even, conc[s, :, 0, :], conc[s, :, ny - 1, :])


def halo(axis, first, second):
    even, lowest, highest = sides(axis)
    above = jnp.where(highest, 0.0, jnp.where(even, first, second))
    below = jnp.where(lowest, 0.0, jnp.where(even, second, first))
    return above, below


def lanes(like):
    return lax.broadcasted_iota(jnp.int32, like, len(like) - 1)


def kept(dims):
    half = dims[-1] // 2
    return (lanes(dims) >= half) == (lax.axis_index("field") == 1)


def turned(value):
    return pltpu.roll(value, value.shape[-1] // 2, value.ndim - 1)


def doubled(value):
    return jnp.where(kept(value.shape), value, turned(value))


def packed(low, high, mask):
    return jnp.where(mask, low, turned(high))


def shifted(value, above, below):
    ny = value.shape[0]
    sub = lax.broadcasted_iota(jnp.int32, value.shape, 0)
    up = jnp.where(sub == ny - 1, above, pltpu.roll(value, ny - 1, 0))
    down = jnp.where(sub == 0, below, pltpu.roll(value, 1, 0))
    return up, down


def means(gamma, x1, x2, y1, y2):
    nx, ny, nz = gamma.shape
    last = x1.shape[0] - 1
    lane = lanes((ny, nz))
    x_above, x_below = halo("gx", x1[last], x2[last])
    y_above, y_below = halo("gy", y1[last], y2[last])
    result = []
    for x in range(nx):
        g = gamma[x]
        pairs = [
            (
                x_above if x == nx - 1 else gamma[x + 1],
                x_below if x == 0 else gamma[x - 1],
            ),
            shifted(g, y_above[x : x + 1], y_below[x : x + 1]),
            (
                jnp.where(lane == nz - 1, 0.0, pltpu.roll(g, nz - 1, 1)),
                jnp.where(lane == 0, 0.0, pltpu.roll(g, 1, 1)),
            ),
        ]
        result.append([(0.5 * (g + up), 0.5 * (g + down)) for up, down in pairs])
    return result


def stencil(pairs, drifts, top, bottom):
    total = sum(up + down for up, down in pairs)
    coef = [(1.0 - total) * LOG2E]
    for (up, down), drift in zip(pairs, drifts):
        coef += [(up + drift) * LOG2E, (down - drift) * LOG2E]
    coef[5] = jnp.where(top, 0.0, coef[5])
    coef[6] = jnp.where(bottom, 0.0, coef[6])
    return coef


def move(conc, s, coefs, x1, x2, y1, y2, along_z):
    nx = conc.shape[1]
    x_above, x_below = halo("gx", x1[s], x2[s])
    y_above, y_below = halo("gy", y1[s], y2[s])
    for x in range(nx):
        centre, xu, xd, yu, yd, zu, zd = coefs[x]
        p = conc[s, x]
        px_up = x_above if x == nx - 1 else conc[s, x + 1]
        px_down = x_below if x == 0 else conc[s, x - 1]
        py_up, py_down = shifted(p, y_above[x : x + 1], y_below[x : x + 1])
        pz_up, pz_down = along_z(p, s * nx + x)
        yield (centre * p + (xu * px_up + xd * px_down)) + (
            (yu * py_up + yd * py_down) + (zu * pz_up + zd * pz_down)
        )


def whole_z(p, item):
    nz = p.shape[1]
    return pltpu.roll(p, nz - 1, 1), pltpu.roll(p, 1, 1)


def chemistry(state, gather, scatter):
    ns, cells = state.shape
    tiles = cells // TILE
    table, net = gather[...][:, : 3 * ns], scatter[...]
    nr = table.shape[0] // 2
    steps = SUBSTEPS * tiles
    lag = tiles // 2
    both, change = {}, {}

    def cut(t):
        return slice(t % tiles * TILE, (t % tiles + 1) * TILE)

    for t in range(steps + 2 * lag):
        done = t - 2 * lag
        if done >= 0:
            u = state[:, cut(done)] + change.pop(done)
            state[:, cut(done)] = u
        if t < steps:
            if done < 0:
                u = state[:, cut(t)]
            sp = jnp.maximum(u, jnp.log2(1.0 + jnp.exp2(jnp.minimum(u, 120.0))))
            hi, lo = split(sp)
            both[t] = jnp.dot(
                table,
                jnp.concatenate([hi, lo, hi], axis=0),
                preferred_element_type=jnp.float32,
            )
        ready = t - lag
        if 0 <= ready < steps:
            pair = both.pop(ready).reshape(nr // 8, 2, 8, TILE)
            hi, lo = split((pair[:, 0] * pair[:, 1]).reshape(nr, TILE))
            change[ready] = jnp.dot(
                net, jnp.concatenate([hi, lo], axis=0), preferred_element_type=jnp.float32
            )


def react(rows, state, gather, scatter):
    ns = state.shape[0]
    nz = rows.shape[1]
    stride = rows.shape[0] // ns
    chunks = state.shape[1] // nz
    for j in range(chunks):
        state[:, j * nz : (j + 1) * nz] = rows[pl.ds(j, ns, stride=stride), :]
    chemistry(state, gather, scatter)
    for j in range(chunks):
        rows[pl.ds(j, ns, stride=stride), :] = state[:, j * nz : (j + 1) * nz] * LN2


def scratch(ns, nx, ny, nz):
    stride = roundup(nx * ny, 32) + 1
    return [
        pltpu.VMEM((ns * stride, nz), jnp.float32),
        pltpu.VMEM((ns, nx * ny * nz), jnp.float32),
    ]


def mixing(pairs, count, mix_rate):
    ns, get = pairs
    spread, energy = jnp.zeros_like(mix_rate), jnp.zeros_like(mix_rate)
    for s in range(ns):
        a, b = get(s)
        mean = (a + b) * (1.0 / count)
        meansq = (a * a + b * b) * (1.0 / count)
        spread = spread + (meansq - mean * mean)
        energy = energy + meansq
    decay = jnp.exp(-0.5 * (mix_rate * (1.0 + spread / (1.0 + energy))))
    for s in range(ns):
        a, b = get(s)
        mean = (a + b) * (1.0 / count)
        yield mean + (a - mean) * decay, mean + (b - mean) * decay


def faces_kernel(conc_in, gamma_in, x1, x2, y1, y2, conc, gamma, sems):
    ns = conc.shape[0]
    copies = [
        pltpu.make_async_copy(conc_in, conc, sems.at[0]),
        pltpu.make_async_copy(gamma_in, gamma, sems.at[1]),
    ]
    for copy in copies:
        copy.start()
    for copy in copies:
        copy.wait()
    for s in range(ns):
        send_faces(conc, s, x1, x2, y1, y2, s)
    send_faces(gamma, 0, x1, x2, y1, y2, ns)


def tables_kernel(ns, reactions, rates, gather, scatter):
    nr = reactions.shape[1]
    depth = gather.shape[1]
    row = lax.broadcasted_iota(jnp.int32, (depth, nr), 0)
    scalar, part = lax.rem(row, ns), lax.div(row, ns)
    k = rates[...] * (CHEM_STEP * LN2)
    k_hi = k.astype(jnp.bfloat16).astype(jnp.float32)
    k_lo = k - k_hi

    def column(c):
        return jnp.where(scalar == reactions[c : c + 1, :], 1.0, 0.0)

    first, second, third, fourth = (column(c) for c in range(4))
    weight = jnp.where(part < 2, k_hi, jnp.where(part == 2, k_lo, 0.0))
    both = jnp.concatenate(
        [first * weight, second * jnp.where(part < 2, 1.0, 0.0)], axis=1
    ).T
    for j in range(nr // 8):
        block = [both[c + 8 * j : c + 8 * j + 8, :] for c in (0, nr)]
        gather[16 * j : 16 * j + 16, :] = jnp.concatenate(block, axis=0).astype(jnp.bfloat16)
    net = (third + fourth - first - second)[:ns].astype(jnp.bfloat16)
    scatter[...] = jnp.concatenate([net, net], axis=1)


def prepare_kernel(
    ns, reactions, rates, gamma, velocity, wiener, mix_rate,
    gather, scatter, drift, amp, speed, noise, noise_out, mix_packed, mix_doubled
):
    tables_kernel(ns, reactions, rates, gather, scatter)
    nx = gamma.shape[1]
    own = kept(gamma.shape[2:])
    for x in range(nx):
        root = jnp.sqrt(2.0 * gamma[0, x])
        amp[x] = doubled(root)
        mix_doubled[x] = doubled(mix_rate[x])
        for d in range(3):
            drift[d, x] = 0.5 * (root * wiener[0, d, 0, x] - velocity[d, x])
            speed[d, x] = doubled(velocity[d, x])
            noise[d, x] = wiener[1, d, 0, x]
    for x in range(nx // 2):
        mix_packed[x] = packed(mix_rate[x], mix_rate[x + nx // 2], own)
        for d in range(3):
            noise_out[d * (nx // 2) + x] = packed(
                wiener[1, d, 0, x], wiener[1, d, 0, x + nx // 2], jnp.logical_not(own)
            )


def leave_kernel(conc, x1, x2, y1, y2, gamma, drift, mine, theirs):
    ns, nx, ny, nz = conc.shape
    own = kept((ny, nz))
    lane = lanes((ny, nz))
    pairs = means(gamma.at[0], x1, x2, y1, y2)
    coefs = [
        stencil(pairs[x], [drift[d, x] for d in range(3)], lane == nz - 1, lane == 0)
        for x in range(nx)
    ]
    for s in range(ns):
        moved = list(move(conc, s, coefs, x1, x2, y1, y2, whole_z))
        for x in range(nx // 2):
            mine[s, x] = packed(moved[x], moved[x + nx // 2], own)
            theirs[s, x] = packed(moved[x], moved[x + nx // 2], jnp.logical_not(own))


def coefs_kernel(gamma, x1, x2, y1, y2, ups, downs):
    pairs = means(gamma.at[0], x1, x2, y1, y2)
    for x, plane in enumerate(pairs):
        for d, (up, down) in enumerate(plane):
            ups[d, x] = doubled(up)
            downs[d, x] = doubled(down)


def first_kernel(
    count, mine, theirs, gather, scatter, mix_rate, noise_out,
    conc, x1, x2, y1, y2, side, rows, state
):
    ns, nx, ny, nz = conc.shape
    half = nx // 2
    stride = rows.shape[0] // ns
    own = kept((ny, nz))
    is_first = lax.axis_index("field") == 0

    def place(s, field, x):
        start = s * stride + (field * half + x) * ny
        return slice(start, start + ny)

    for s in range(ns):
        for x in range(half):
            rows[place(s, 0, x), :] = mine[s, x]
            rows[place(s, 1, x), :] = theirs[s, x]
    react(rows, state, gather, scatter)
    for x in range(half):
        mixed = mixing(
            (ns, lambda s: (rows[place(s, 0, x), :], rows[place(s, 1, x), :])),
            count,
            mix_rate[x],
        )
        for s, (a, b) in enumerate(mixed):
            conc[s, x] = packed(a, b, own)
            conc[s, x + half] = jnp.where(own, turned(a), b)
    per = nz // 2
    lane = lax.rem(lanes((ny, nz)), per)
    parts = side.shape[0] - noise_out.shape[0]
    for part in range(parts):
        column = jnp.zeros((ny, nz), jnp.float32)
        for item in range(part * per, min(ns * nx, (part + 1) * per)):
            j = item % per
            shift = jnp.where(is_first, (j + per + 1) % nz, j)
            value = pltpu.roll(conc[item // nx, item % nx], shift, 1)
            column = jnp.where(lane == j, value, column)
        side[part] = column
    side[parts:] = noise_out[...]
    for s in range(ns):
        send_faces(conc, s, x1, x2, y1, y2, s)


def second_kernel(
    count, conc, x1, x2, y1, y2, side, ups, downs, amp, speed, noise, gather, scatter, mix_rate,
    mine, theirs, rows, state
):
    ns, nx, ny, nz = conc.shape
    half, per = nx // 2, nz // 2
    stride = rows.shape[0] // ns
    own = kept((ny, nz))
    is_first = lax.axis_index("field") == 0
    lane = lax.rem(lanes((ny, nz)), per)
    at_top, at_bottom = lane == per - 1, lane == 0
    top = jnp.logical_and(at_top, jnp.logical_not(is_first))
    bottom = jnp.logical_and(at_bottom, is_first)
    parts = side.shape[0] - 3 * half

    def half_z(p, item):
        j = item % per
        shift = jnp.where(is_first, per - 1 - j, (nz - j) % nz)
        edge = pltpu.roll(side[item // per], shift, 1)
        up, down = whole_z(p, item)
        return jnp.where(at_top, edge, up), jnp.where(at_bottom, edge, down)

    coefs = []
    for x in range(nx):
        drifts = []
        for d in range(3):
            got = side[parts + d * half + x % half]
            other = turned(got) if x < half else got
            drifts.append(0.5 * (amp[x] * jnp.where(own, noise[d, x], other) - speed[d, x]))
        pairs = [(ups[d, x], downs[d, x]) for d in range(3)]
        coefs.append(stencil(pairs, drifts, top, bottom))
    for s in range(ns):
        for x, moved in enumerate(move(conc, s, coefs, x1, x2, y1, y2, half_z)):
            rows[s * stride + x * ny : s * stride + (x + 1) * ny, :] = moved
    react(rows, state, gather, scatter)

    def field_pair(x):
        def get(s):
            a = rows[s * stride + x * ny : s * stride + (x + 1) * ny, :]
            return a, turned(a)

        return get

    for x in range(half):
        low = mixing((ns, field_pair(x)), count, mix_rate[x])
        high = mixing((ns, field_pair(x + half)), count, mix_rate[x + half])
        for s, ((a, _), (b, _)) in enumerate(zip(low, high)):
            mine[s, x] = a
            mine[s, x + half] = b
            theirs[s, x] = packed(a, b, jnp.logical_not(own))


def join_kernel(mine, theirs, out):
    ns, nx, ny, nz = mine.shape
    half = nx // 2
    own = kept((ny, nz))
    for s in range(ns):
        for x in range(half):
            out[s, x] = packed(mine[s, x], theirs[s, x], own)
            out[s, x + half] = jnp.where(own, mine[s, x + half], theirs[s, x])


def step_kernel(
    step, conc, x1, x2, y1, y2, gamma, gx1, gx2, gy1, gy2, velocity, wiener, gather, scatter,
    out, rows, state
):
    ns, nx, ny, nz = conc.shape
    stride = rows.shape[0] // ns
    lane = lanes((ny, nz))
    pairs = means(gamma.at[0], gx1, gx2, gy1, gy2)
    coefs = []
    for x in range(nx):
        amp = jnp.sqrt(2.0 * gamma[0, x])
        drifts = [0.5 * (amp * wiener[step, d, 0, x] - velocity[d, x]) for d in range(3)]
        coefs.append(stencil(pairs[x], drifts, lane == nz - 1, lane == 0))
    for s in range(ns):
        for x, moved in enumerate(move(conc, s, coefs, x1, x2, y1, y2, whole_z)):
            rows[s * stride + x * ny : s * stride + (x + 1) * ny, :] = moved
    react(rows, state, gather, scatter)
    for s in range(ns):
        for x in range(nx):
            out[s, x] = rows[s * stride + x * ny : s * stride + (x + 1) * ny, :]


def closure(first, second, count, mix_rate):
    mean = first / count
    meansq = second / count
    spread = jnp.sum(meansq - mean * mean, axis=0)
    energy = jnp.sum(meansq, axis=0)
    omega = mix_rate * (1.0 + spread / (1.0 + energy))
    return (mean, jnp.exp(-0.5 * omega))


def on_device(concentrations, velocity, diffusivity, wiener, mix_rate, rate_constants, reactions):
    ns, nx, ny, nz = concentrations.shape[1:]
    nr = reactions.shape[0]
    count = lax.axis_size("field")
    rates = rate_constants.reshape(1, nr)
    table_shapes = [
        shape_of(2 * nr, 128, dtype=jnp.bfloat16), shape_of(ns, 2 * nr, dtype=jnp.bfloat16)
    ]
    face_dims = [(ny, nz), (ny, nz), (nx, nz), (nx, nz)]
    faces = [shape_of(ns, *d) for d in face_dims]
    block = shape_of(ns, nx, ny, nz)
    *sent, conc, gamma = call(
        faces_kernel, 4,
        [shape_of(ns + 1, *d) for d in face_dims] + [block, shape_of(1, nx, ny, nz)],
        *(pltpu.with_memory_space_constraint(a, pltpu.HBM) for a in (concentrations[0], diffusivity[None])),
        in_specs=[HBM] * 2, scratch_shapes=[pltpu.SemaphoreType.DMA((2,))],
    )
    halos = exchange(*sent)
    if count == 2 and STEPS == 2 and nx % 2 == 0 and nz == 128:
        half = shape_of(ns, nx // 2, ny, nz)
        partner = [(0, 1), (1, 0)]
        vectors, planes = shape_of(3, nx, ny, nz), shape_of(nx, ny, nz)
        noise_dims = 3 * (nx // 2)
        gather, scatter, drift, amp, speed, noise, noise_out, mix_packed, mix_doubled = call(
            functools.partial(prepare_kernel, ns), 4,
            table_shapes
            + [vectors, planes, vectors, vectors, shape_of(noise_dims, ny, nz)]
            + [shape_of(nx // 2, ny, nz), planes],
            reactions.T, rates, gamma, velocity, wiener, mix_rate,
        )
        mine, theirs = call(leave_kernel, 4, [half, half], conc, *halos, gamma, drift)
        theirs = lax.ppermute(theirs, "field", partner)
        ups, downs = call(coefs_kernel, 4, [vectors, vectors], gamma, *halos)
        parts = -(-ns * nx // (nz // 2))
        conc, *sent, side = call(
            functools.partial(first_kernel, count), 8,
            [block] + faces + [shape_of(parts + noise_dims, ny, nz)],
            mine, theirs, gather, scatter, mix_packed, noise_out,
            scratch_shapes=scratch(ns, nx, ny, nz),
        )
        side = lax.ppermute(side, "field", partner)
        halos = exchange(*sent)
        mine, theirs = call(
            functools.partial(second_kernel, count), 8, [block, half],
            conc, *halos, side, ups, downs, amp, speed, noise, gather, scatter, mix_doubled,
            scratch_shapes=scratch(ns, nx, ny, nz),
        )
        theirs = lax.ppermute(theirs, "field", partner)
        (out,) = call(join_kernel, 4, [block], mine, theirs)
        return out[None]
    gather, scatter = call(
        functools.partial(tables_kernel, ns), 2, table_shapes, reactions.T, rates
    )
    gamma_halos = halos
    for step_index in range(STEPS):
        (reacted,) = call(
            functools.partial(step_kernel, step_index), 8, [block],
            conc, *halos, gamma, *gamma_halos, velocity, wiener, gather, scatter,
            scratch_shapes=scratch(ns, nx, ny, nz),
        )
        first = lax.psum(reacted, "field")
        second = lax.psum(reacted * reacted, "field")
        mean, decay = closure(first, second, count, mix_rate)
        conc = mean + (reacted - mean) * decay
        if step_index < STEPS - 1:
            sent = picked(sides("gx")[0], conc[:, 0], conc[:, -1])
            sent += picked(sides("gy")[0], conc[:, :, 0], conc[:, :, -1])
            halos = exchange(*sent)
    return conc[None]


def solution(mesh):
    return jax.shard_map(
        on_device,
        mesh=mesh,
        in_specs=(
            P("field", None, "gx", "gy", None),
            P(None, "gx", "gy", None),
            P("gx", "gy", None),
            P(None, None, "field", "gx", "gy", None),
            P("gx", "gy", None),
            P(),
            P(),
        ),
        out_specs=P("field", None, "gx", "gy", None),
        check_vma=False,
    )
```

```python
import functools

import jax
import jax.numpy as jnp
from jax import lax
from jax.experimental import pallas as pl
from jax.experimental.pallas import tpu as pltpu
from jax.sharding import PartitionSpec as P


SUBSTEPS = 12
STEPS = 2
CHEM_STEP = 0.04
LOG2E = 1.4426950408889634
LN2 = 0.6931471805599453
TILE = 256
DIRECT = 2
VMEM = pl.BlockSpec(memory_space=pltpu.VMEM)
HBM = pl.BlockSpec(memory_space=pltpu.HBM)


def roundup(n, m):
    return (n + m - 1) // m * m


def split(x):
    hi = x.astype(jnp.bfloat16)
    lo = (x - hi.astype(jnp.float32)).astype(jnp.bfloat16)
    return hi, lo


def shape_of(*dims, dtype=jnp.float32):
    return jax.ShapeDtypeStruct(dims, dtype)


def call(kernel, mib, out_shape, *args, in_specs=None, scratch_shapes=()):
    return pl.pallas_call(
        kernel,
        out_shape=out_shape,
        in_specs=in_specs or [VMEM] * len(args),
        out_specs=[VMEM] * len(out_shape),
        scratch_shapes=scratch_shapes,
        compiler_params=pltpu.CompilerParams(vmem_limit_bytes=mib * 2**20),
    )(*args)


def swaps(count):
    pairs = [[(i, i + 1) for i in range(start, count - 1, 2)] for start in (0, 1)]
    return [(p, sorted(set(range(count)) - {i for q in p for i in q})) for p in pairs]


def swap(value, axis, pairs, rest, other=None):
    both = pairs + [(j, i) for i, j in pairs]
    if other is not None and rest and lax.axis_size(other) % 2 == 0:
        n = lax.axis_size(other)
        joint = [(i * n + k, j * n + k) for i, j in both for k in range(n)]
        joint += [(i * n + k, i * n + k + 1 - 2 * (k % 2)) for i in rest for k in range(n)]
        return lax.ppermute(value, (axis, other), joint)
    if len(rest) == 2:
        both = both + [tuple(rest), tuple(rest[::-1])]
    else:
        both = both + [(i, i) for i in rest]
    return lax.ppermute(value, axis, both)


def exchange(x1, x2, y1, y2):
    (a, rest_a), (b, rest_b) = swaps(lax.axis_size("gx"))
    (c, rest_c), (d, rest_d) = swaps(lax.axis_size("gy"))
    x1 = swap(x1, "gx", a, rest_a, "gy")
    x2 = swap(x2, "gx", b, rest_b, "gy")
    y1 = swap(y1, "gy", c, rest_c)
    y2 = swap(y2, "gy", d, rest_d)
    return x1, x2, y1, y2


def sides(axis):
    here, count = lax.axis_index(axis), lax.axis_size(axis)
    even = lax.rem(here, 2) == 0
    return even, here == 0, here == count - 1


def picked(even, low, high):
    return jnp.where(even, high, low), jnp.where(even, low, high)


def send_faces(conc, s, x1, x2, y1, y2, row):
    nx, ny = conc.shape[-3], conc.shape[-2]
    even, _, _ = sides("gx")
    for ref, x in zip((x1, x2), picked(even, 0, nx - 1)):
        ref[row] = conc[s, x]
    even, _, _ = sides("gy")
    y1[row], y2[row] = picked(even, conc[s, :, 0, :], conc[s, :, ny - 1, :])


def halo(axis, first, second):
    even, lowest, highest = sides(axis)
    above = jnp.where(highest, 0.0, jnp.where(even, first, second))
    below = jnp.where(lowest, 0.0, jnp.where(even, second, first))
    return above, below


def lanes(like):
    return lax.broadcasted_iota(jnp.int32, like, len(like) - 1)


def kept(dims):
    half = dims[-1] // 2
    return (lanes(dims) >= half) == (lax.axis_index("field") == 1)


def turned(value):
    return pltpu.roll(value, value.shape[-1] // 2, value.ndim - 1)


def doubled(value):
    return jnp.where(kept(value.shape), value, turned(value))


def packed(low, high, mask):
    return jnp.where(mask, low, turned(high))


def shifted(value, above, below):
    ny = value.shape[0]
    sub = lax.broadcasted_iota(jnp.int32, value.shape, 0)
    up = jnp.where(sub == ny - 1, above, pltpu.roll(value, ny - 1, 0))
    down = jnp.where(sub == 0, below, pltpu.roll(value, 1, 0))
    return up, down


def means(gamma, x1, x2, y1, y2):
    nx, ny, nz = gamma.shape
    last = x1.shape[0] - 1
    lane = lanes((ny, nz))
    x_above, x_below = halo("gx", x1[last], x2[last])
    y_above, y_below = halo("gy", y1[last], y2[last])
    result = []
    for x in range(nx):
        g = gamma[x]
        pairs = [
            (
                x_above if x == nx - 1 else gamma[x + 1],
                x_below if x == 0 else gamma[x - 1],
            ),
            shifted(g, y_above[x : x + 1], y_below[x : x + 1]),
            (
                jnp.where(lane == nz - 1, 0.0, pltpu.roll(g, nz - 1, 1)),
                jnp.where(lane == 0, 0.0, pltpu.roll(g, 1, 1)),
            ),
        ]
        result.append([(0.5 * (g + up), 0.5 * (g + down)) for up, down in pairs])
    return result


def stencil(pairs, drifts, top, bottom):
    total = sum(up + down for up, down in pairs)
    coef = [(1.0 - total) * LOG2E]
    for (up, down), drift in zip(pairs, drifts):
        coef += [(up + drift) * LOG2E, (down - drift) * LOG2E]
    coef[5] = jnp.where(top, 0.0, coef[5])
    coef[6] = jnp.where(bottom, 0.0, coef[6])
    return coef


def move(conc, s, coefs, x1, x2, y1, y2, along_z):
    nx = conc.shape[1]
    x_above, x_below = halo("gx", x1[s], x2[s])
    y_above, y_below = halo("gy", y1[s], y2[s])
    for x in range(nx):
        centre, xu, xd, yu, yd, zu, zd = coefs[x]
        p = conc[s, x]
        px_up = x_above if x == nx - 1 else conc[s, x + 1]
        px_down = x_below if x == 0 else conc[s, x - 1]
        py_up, py_down = shifted(p, y_above[x : x + 1], y_below[x : x + 1])
        pz_up, pz_down = along_z(p, s * nx + x)
        yield (centre * p + (xu * px_up + xd * px_down)) + (
            (yu * py_up + yd * py_down) + (zu * pz_up + zd * pz_down)
        )


def whole_z(p, item):
    nz = p.shape[1]
    return pltpu.roll(p, nz - 1, 1), pltpu.roll(p, 1, 1)


def second_reactant(sp, index):
    width = index.shape[1]
    pieces = []
    for start in range(0, sp.shape[1], width):
        picked_rows = None
        for low in range(0, sp.shape[0], 8):
            rows = sp[low : low + 8, start : start + width]
            inside = jnp.logical_and(index >= low, index < low + 8)
            got = jnp.take_along_axis(rows, jnp.where(inside, index - low, 0), axis=0)
            picked_rows = got if low == 0 else jnp.where(inside, got, picked_rows)
        pieces.append(picked_rows)
    return jnp.concatenate(pieces, axis=1)


def chemistry(state, gather, scatter, index):
    ns, cells = state.shape
    tiles = cells // TILE
    table, net = gather[...][:, : 3 * ns], scatter[...]
    paired = net.shape[1] // 16 - DIRECT
    steps = SUBSTEPS * tiles
    lag = tiles // 2
    both, direct, change = {}, {}, {}

    def cut(t):
        return slice(t % tiles * TILE, (t % tiles + 1) * TILE)

    for t in range(steps + 2 * lag):
        done = t - 2 * lag
        if done >= 0:
            u = state[:, cut(done)] + change.pop(done)
            state[:, cut(done)] = u
        if t < steps:
            if done < 0:
                u = state[:, cut(t)]
            sp = jnp.maximum(u, jnp.log2(1.0 + jnp.exp2(jnp.minimum(u, 120.0))))
            hi, lo = split(sp)
            both[t] = jnp.dot(
                table,
                jnp.concatenate([hi, lo, hi], axis=0),
                preferred_element_type=jnp.float32,
            )
            direct[t] = [second_reactant(sp, index[j]) for j in range(DIRECT)]
        ready = t - lag
        if 0 <= ready < steps:
            got = both.pop(ready)
            pair = got[: 16 * paired].reshape(paired, 2, 8, TILE)
            rates = [(pair[:, 0] * pair[:, 1]).reshape(8 * paired, TILE)]
            for j, second in enumerate(direct.pop(ready)):
                start = 16 * paired + 8 * j
                rates.append(got[start : start + 8] * second)
            hi, lo = split(jnp.concatenate(rates, axis=0))
            change[ready] = jnp.dot(
                net, jnp.concatenate([hi, lo], axis=0), preferred_element_type=jnp.float32
            )


def react(rows, state, gather, scatter, index):
    ns = state.shape[0]
    nz = rows.shape[1]
    stride = rows.shape[0] // ns
    chunks = state.shape[1] // nz
    for j in range(chunks):
        state[:, j * nz : (j + 1) * nz] = rows[pl.ds(j, ns, stride=stride), :]
    chemistry(state, gather, scatter, index)
    for j in range(chunks):
        rows[pl.ds(j, ns, stride=stride), :] = state[:, j * nz : (j + 1) * nz] * LN2


def scratch(ns, nx, ny, nz):
    stride = roundup(nx * ny, 32) + 1
    return [
        pltpu.VMEM((ns * stride, nz), jnp.float32),
        pltpu.VMEM((ns, nx * ny * nz), jnp.float32),
    ]


def mixing(pairs, count, mix_rate):
    ns, get = pairs
    spread, energy = jnp.zeros_like(mix_rate), jnp.zeros_like(mix_rate)
    for s in range(ns):
        a, b = get(s)
        mean = (a + b) * (1.0 / count)
        meansq = (a * a + b * b) * (1.0 / count)
        spread = spread + (meansq - mean * mean)
        energy = energy + meansq
    decay = jnp.exp(-0.5 * (mix_rate * (1.0 + spread / (1.0 + energy))))
    for s in range(ns):
        a, b = get(s)
        mean = (a + b) * (1.0 / count)
        yield mean + (a - mean) * decay, mean + (b - mean) * decay


def faces_kernel(conc_in, gamma_in, x1, x2, y1, y2, conc, gamma, sems):
    ns = conc.shape[0]
    copies = [
        pltpu.make_async_copy(conc_in, conc, sems.at[0]),
        pltpu.make_async_copy(gamma_in, gamma, sems.at[1]),
    ]
    for copy in copies:
        copy.start()
    for copy in copies:
        copy.wait()
    for s in range(ns):
        send_faces(conc, s, x1, x2, y1, y2, s)
    send_faces(gamma, 0, x1, x2, y1, y2, ns)


def tables_kernel(ns, reactions, rates, gather, scatter, index):
    nr = reactions.shape[1]
    depth = gather.shape[1]
    paired = nr // 8 - DIRECT
    row = lax.broadcasted_iota(jnp.int32, (depth, nr), 0)
    scalar, part = lax.rem(row, ns), lax.div(row, ns)
    k = rates[...] * (CHEM_STEP * LN2)
    k_hi = k.astype(jnp.bfloat16).astype(jnp.float32)
    k_lo = k - k_hi

    def column(c):
        return jnp.where(scalar == reactions[c : c + 1, :], 1.0, 0.0)

    first, second, third, fourth = (column(c) for c in range(4))
    weight = jnp.where(part < 2, k_hi, jnp.where(part == 2, k_lo, 0.0))
    both = jnp.concatenate(
        [first * weight, second * jnp.where(part < 2, 1.0, 0.0)], axis=1
    ).T
    for j in range(paired):
        block = [both[c + 8 * j : c + 8 * j + 8, :] for c in (0, nr)]
        gather[16 * j : 16 * j + 16, :] = jnp.concatenate(block, axis=0).astype(jnp.bfloat16)
    gather[16 * paired :, :] = both[8 * paired : nr, :].astype(jnp.bfloat16)
    partner = jnp.broadcast_to(reactions[1:2, :].astype(jnp.float32), (depth, nr))
    partner = jnp.concatenate([partner, partner], axis=1).T
    for j in range(DIRECT):
        start = 8 * (paired + j)
        index[j] = partner[start : start + 8, :].astype(jnp.int32)
    net = (third + fourth - first - second)[:ns].astype(jnp.bfloat16)
    scatter[...] = jnp.concatenate([net, net], axis=1)


def prepare_kernel(
    ns, reactions, rates, gamma, velocity, wiener, mix_rate,
    gather, scatter, index, drift, amp, speed, noise, noise_out, mix_packed, mix_doubled
):
    tables_kernel(ns, reactions, rates, gather, scatter, index)
    nx = gamma.shape[1]
    own = kept(gamma.shape[2:])
    for x in range(nx):
        root = jnp.sqrt(2.0 * gamma[0, x])
        amp[x] = doubled(root)
        mix_doubled[x] = doubled(mix_rate[x])
        for d in range(3):
            drift[d, x] = 0.5 * (root * wiener[0, d, 0, x] - velocity[d, x])
            speed[d, x] = doubled(velocity[d, x])
            noise[d, x] = wiener[1, d, 0, x]
    for x in range(nx // 2):
        mix_packed[x] = packed(mix_rate[x], mix_rate[x + nx // 2], own)
        for d in range(3):
            noise_out[d * (nx // 2) + x] = packed(
                wiener[1, d, 0, x], wiener[1, d, 0, x + nx // 2], jnp.logical_not(own)
            )


def leave_kernel(conc, x1, x2, y1, y2, gamma, drift, mine, theirs):
    ns, nx, ny, nz = conc.shape
    own = kept((ny, nz))
    lane = lanes((ny, nz))
    pairs = means(gamma.at[0], x1, x2, y1, y2)
    coefs = [
        stencil(pairs[x], [drift[d, x] for d in range(3)], lane == nz - 1, lane == 0)
        for x in range(nx)
    ]
    for s in range(ns):
        moved = list(move(conc, s, coefs, x1, x2, y1, y2, whole_z))
        for x in range(nx // 2):
            mine[s, x] = packed(moved[x], moved[x + nx // 2], own)
            theirs[s, x] = packed(moved[x], moved[x + nx // 2], jnp.logical_not(own))


def coefs_kernel(gamma, x1, x2, y1, y2, ups, downs):
    pairs = means(gamma.at[0], x1, x2, y1, y2)
    for x, plane in enumerate(pairs):
        for d, (up, down) in enumerate(plane):
            ups[d, x] = doubled(up)
            downs[d, x] = doubled(down)


def first_kernel(
    count, mine, theirs, gather, scatter, index, mix_rate, noise_out,
    conc, x1, x2, y1, y2, side, rows, state
):
    ns, nx, ny, nz = conc.shape
    half = nx // 2
    stride = rows.shape[0] // ns
    own = kept((ny, nz))
    is_first = lax.axis_index("field") == 0

    def place(s, field, x):
        start = s * stride + (field * half + x) * ny
        return slice(start, start + ny)

    for s in range(ns):
        for x in range(half):
            rows[place(s, 0, x), :] = mine[s, x]
            rows[place(s, 1, x), :] = theirs[s, x]
    react(rows, state, gather, scatter, index)
    for x in range(half):
        mixed = mixing(
            (ns, lambda s: (rows[place(s, 0, x), :], rows[place(s, 1, x), :])),
            count,
            mix_rate[x],
        )
        for s, (a, b) in enumerate(mixed):
            conc[s, x] = packed(a, b, own)
            conc[s, x + half] = jnp.where(own, turned(a), b)
    per = nz // 2
    lane = lax.rem(lanes((ny, nz)), per)
    parts = side.shape[0] - noise_out.shape[0]
    for part in range(parts):
        column = jnp.zeros((ny, nz), jnp.float32)
        for item in range(part * per, min(ns * nx, (part + 1) * per)):
            j = item % per
            shift = jnp.where(is_first, (j + per + 1) % nz, j)
            value = pltpu.roll(conc[item // nx, item % nx], shift, 1)
            column = jnp.where(lane == j, value, column)
        side[part] = column
    side[parts:] = noise_out[...]
    for s in range(ns):
        send_faces(conc, s, x1, x2, y1, y2, s)


def second_kernel(
    count, conc, x1, x2, y1, y2, side, ups, downs, amp, speed, noise, gather, scatter, index, mix_rate,
    mine, theirs, rows, state
):
    ns, nx, ny, nz = conc.shape
    half, per = nx // 2, nz // 2
    stride = rows.shape[0] // ns
    own = kept((ny, nz))
    is_first = lax.axis_index("field") == 0
    lane = lax.rem(lanes((ny, nz)), per)
    at_top, at_bottom = lane == per - 1, lane == 0
    top = jnp.logical_and(at_top, jnp.logical_not(is_first))
    bottom = jnp.logical_and(at_bottom, is_first)
    parts = side.shape[0] - 3 * half

    def half_z(p, item):
        j = item % per
        shift = jnp.where(is_first, per - 1 - j, (nz - j) % nz)
        edge = pltpu.roll(side[item // per], shift, 1)
        up, down = whole_z(p, item)
        return jnp.where(at_top, edge, up), jnp.where(at_bottom, edge, down)

    coefs = []
    for x in range(nx):
        drifts = []
        for d in range(3):
            got = side[parts + d * half + x % half]
            other = turned(got) if x < half else got
            drifts.append(0.5 * (amp[x] * jnp.where(own, noise[d, x], other) - speed[d, x]))
        pairs = [(ups[d, x], downs[d, x]) for d in range(3)]
        coefs.append(stencil(pairs, drifts, top, bottom))
    for s in range(ns):
        for x, moved in enumerate(move(conc, s, coefs, x1, x2, y1, y2, half_z)):
            rows[s * stride + x * ny : s * stride + (x + 1) * ny, :] = moved
    react(rows, state, gather, scatter, index)

    def field_pair(x):
        def get(s):
            a = rows[s * stride + x * ny : s * stride + (x + 1) * ny, :]
            return a, turned(a)

        return get

    for x in range(half):
        low = mixing((ns, field_pair(x)), count, mix_rate[x])
        high = mixing((ns, field_pair(x + half)), count, mix_rate[x + half])
        for s, ((a, _), (b, _)) in enumerate(zip(low, high)):
            mine[s, x] = a
            mine[s, x + half] = b
            theirs[s, x] = packed(a, b, jnp.logical_not(own))


def join_kernel(mine, theirs, out):
    ns, nx, ny, nz = mine.shape
    half = nx // 2
    own = kept((ny, nz))
    for s in range(ns):
        for x in range(half):
            out[s, x] = packed(mine[s, x], theirs[s, x], own)
            out[s, x + half] = jnp.where(own, mine[s, x + half], theirs[s, x])


def step_kernel(
    step, conc, x1, x2, y1, y2, gamma, gx1, gx2, gy1, gy2, velocity, wiener, gather, scatter, index,
    out, rows, state
):
    ns, nx, ny, nz = conc.shape
    stride = rows.shape[0] // ns
    lane = lanes((ny, nz))
    pairs = means(gamma.at[0], gx1, gx2, gy1, gy2)
    coefs = []
    for x in range(nx):
        amp = jnp.sqrt(2.0 * gamma[0, x])
        drifts = [0.5 * (amp * wiener[step, d, 0, x] - velocity[d, x]) for d in range(3)]
        coefs.append(stencil(pairs[x], drifts, lane == nz - 1, lane == 0))
    for s in range(ns):
        for x, moved in enumerate(move(conc, s, coefs, x1, x2, y1, y2, whole_z)):
            rows[s * stride + x * ny : s * stride + (x + 1) * ny, :] = moved
    react(rows, state, gather, scatter, index)
    for s in range(ns):
        for x in range(nx):
            out[s, x] = rows[s * stride + x * ny : s * stride + (x + 1) * ny, :]


def closure(first, second, count, mix_rate):
    mean = first / count
    meansq = second / count
    spread = jnp.sum(meansq - mean * mean, axis=0)
    energy = jnp.sum(meansq, axis=0)
    omega = mix_rate * (1.0 + spread / (1.0 + energy))
    return (mean, jnp.exp(-0.5 * omega))


def on_device(concentrations, velocity, diffusivity, wiener, mix_rate, rate_constants, reactions):
    ns, nx, ny, nz = concentrations.shape[1:]
    nr = reactions.shape[0]
    count = lax.axis_size("field")
    rates = rate_constants.reshape(1, nr)
    table_shapes = [
        shape_of(2 * nr - 8 * DIRECT, 128, dtype=jnp.bfloat16),
        shape_of(ns, 2 * nr, dtype=jnp.bfloat16),
        shape_of(DIRECT, 8, 128, dtype=jnp.int32),
    ]
    face_dims = [(ny, nz), (ny, nz), (nx, nz), (nx, nz)]
    faces = [shape_of(ns, *d) for d in face_dims]
    block = shape_of(ns, nx, ny, nz)
    *sent, conc, gamma = call(
        faces_kernel, 4,
        [shape_of(ns + 1, *d) for d in face_dims] + [block, shape_of(1, nx, ny, nz)],
        *(pltpu.with_memory_space_constraint(a, pltpu.HBM) for a in (concentrations[0], diffusivity[None])),
        in_specs=[HBM] * 2, scratch_shapes=[pltpu.SemaphoreType.DMA((2,))],
    )
    halos = exchange(*sent)
    if count == 2 and STEPS == 2 and nx % 2 == 0 and nz == 128:
        half = shape_of(ns, nx // 2, ny, nz)
        partner = [(0, 1), (1, 0)]
        vectors, planes = shape_of(3, nx, ny, nz), shape_of(nx, ny, nz)
        noise_dims = 3 * (nx // 2)
        *tables, drift, amp, speed, noise, noise_out, mix_packed, mix_doubled = call(
            functools.partial(prepare_kernel, ns), 4,
            table_shapes
            + [vectors, planes, vectors, vectors, shape_of(noise_dims, ny, nz)]
            + [shape_of(nx // 2, ny, nz), planes],
            reactions.T, rates, gamma, velocity, wiener, mix_rate,
        )
        mine, theirs = call(leave_kernel, 4, [half, half], conc, *halos, gamma, drift)
        theirs = lax.ppermute(theirs, "field", partner)
        ups, downs = call(coefs_kernel, 4, [vectors, vectors], gamma, *halos)
        parts = -(-ns * nx // (nz // 2))
        conc, *sent, side = call(
            functools.partial(first_kernel, count), 8,
            [block] + faces + [shape_of(parts + noise_dims, ny, nz)],
            mine, theirs, *tables, mix_packed, noise_out,
            scratch_shapes=scratch(ns, nx, ny, nz),
        )
        side = lax.ppermute(side, "field", partner)
        halos = exchange(*sent)
        mine, theirs = call(
            functools.partial(second_kernel, count), 8, [block, half],
            conc, *halos, side, ups, downs, amp, speed, noise, *tables, mix_doubled,
            scratch_shapes=scratch(ns, nx, ny, nz),
        )
        theirs = lax.ppermute(theirs, "field", partner)
        (out,) = call(join_kernel, 4, [block], mine, theirs)
        return out[None]
    tables = call(functools.partial(tables_kernel, ns), 2, table_shapes, reactions.T, rates)
    gamma_halos = halos
    for step_index in range(STEPS):
        (reacted,) = call(
            functools.partial(step_kernel, step_index), 8, [block],
            conc, *halos, gamma, *gamma_halos, velocity, wiener, *tables,
            scratch_shapes=scratch(ns, nx, ny, nz),
        )
        first = lax.psum(reacted, "field")
        second = lax.psum(reacted * reacted, "field")
        mean, decay = closure(first, second, count, mix_rate)
        conc = mean + (reacted - mean) * decay
        if step_index < STEPS - 1:
            sent = picked(sides("gx")[0], conc[:, 0], conc[:, -1])
            sent += picked(sides("gy")[0], conc[:, :, 0], conc[:, :, -1])
            halos = exchange(*sent)
    return conc[None]


def solution(mesh):
    return jax.shard_map(
        on_device,
        mesh=mesh,
        in_specs=(
            P("field", None, "gx", "gy", None),
            P(None, "gx", "gy", None),
            P("gx", "gy", None),
            P(None, None, "field", "gx", "gy", None),
            P("gx", "gy", None),
            P(),
            P(),
        ),
        out_specs=P("field", None, "gx", "gy", None),
        check_vma=False,
    )
```
